256 devices in a mesh: seq: 16 (over z, x_lo), head: 16 (over y, x_hi, core).
Axes of the slice: x: 4 (x_hi: 2, x_lo: 2; x = x_hi * 2 + x_lo), y: 4, z: 8, core: 2. Of those that a mesh axis runs over, the one named last changes fastest.
Arguments:
- queries: bfloat16 [8192, 6144], P('seq', 'head'), may hold values from -10 to 10
- keys: bfloat16 [8192, 6144], P('seq', 'head'), may hold values from -10 to 10
- values: bfloat16 [8192, 6144], P('seq', 'head'), may hold values from -6 to 6
- frame_of_block: int32 [32], P('seq'), may hold values from 0 to 15, never falling along the last dimension, each value on 1 to 4 neighbouring positions
- pair_mask: int32 [32, 32], P('seq'), may hold values 0 or 1
- w_out: bfloat16 [6144, 6144], P('head', 'seq'), may hold values from -0.4375 to 0.4375
Outputs:
- projected: bfloat16 [8192, 6144], P('seq', 'head')
The draws below stay inside these ranges and needn't reach their ends.
Inputs may be any that keep to these rules, and one draw needn't show every extreme that they name: `frame_of_block`: frame ids never fall along the blocks, every frame spans 1 to 4 consecutive blocks.
All inputs are finite; a program needn't handle non-finite values. No bound on the sum of `pair_mask` on one device may be relied on, other than what follows from the above.
Results may differ from the reference program's by a relative error of at most 0.015.
Values may be sent and summed in bfloat16 or wider, within the bound.
A program may use at most 192 MiB of HBM per device.

```python
import math
import jax
import jax.numpy as jnp
import numpy as np
from jax import lax

D = 6144
H = 48
HD = 128
BLK = 256
TOK_DEV = 512
TOKENS = 8192
NBLK = 32
FRAMES = 16


def joint_draw(key):
    width = H * HD
    q_draw = jnp.clip(1.5 * jax.random.normal(jax.random.fold_in(key, 101), (TOKENS, width), jnp.float32), -6.0, 6.0)
    k_draw = jnp.clip(1.5 * jax.random.normal(jax.random.fold_in(key, 202), (TOKENS, width), jnp.float32), -6.0, 6.0)
    return (q_draw, k_draw)


def draw_queries(key, part):
    return joint_draw(key)[0].astype(jnp.bfloat16)


def draw_keys(key, part):
    return joint_draw(key)[1].astype(jnp.bfloat16)


def touch_ends(result, stream_key, least, largest):
    spot = [jax.random.randint(jax.random.fold_in(stream_key, axis), (), 0, length) for axis, length in enumerate(result.shape)]
    main_axis = result.shape.index(max(result.shape))
    beside = spot[:main_axis] + [(spot[main_axis] + 1) % result.shape[main_axis]] + spot[main_axis + 1:]
    return result.at[tuple(spot)].set(least).at[tuple(beside)].set(largest)


def shard_levels(own_key, extent, shards, low, largest):
    factor_of, own = 1.0, jax.random.fold_in(own_key, 6)
    for dim, parts in shards:
        steps = jnp.exp(jax.random.uniform(jax.random.fold_in(own, dim), (parts,), jnp.float32, low / len(shards), largest / len(shards)))
        factor_of = factor_of * jnp.repeat(steps, extent[dim] // parts).reshape([-1 if axis == dim else 1 for axis in range(len(extent))])
    return factor_of


def length_profile(count, total, most, slope):
    weights = [(1 << 20) // math.isqrt(standing ** slope) + 1 for standing in range(2, count + 1)]
    spare, given = total - most - (count - 1), [1] * (count - 1)
    while spare > 0:
        movable = [i for i in range(count - 1) if given[i] < most]
        mass, left = sum([weights[i] for i in movable]), spare
        for i in movable:
            more = min(most - given[i], max(1, left * weights[i] // mass), spare)
            given[i] = given[i] + more
            spare = spare - more
    return np.array([most] + given)


def uneven_parts(key, amount, total, reach, skew):
    if amount == 2:
        one = jax.random.randint(key, (), max(1, total - reach), min(reach, total - 1) + 1)
        return jnp.stack([one, total - one])
    tallies = jnp.asarray(length_profile(amount, total, reach, skew), jnp.int32)
    twos = (amount - 1) // 2
    giver, sink = tallies[1:1 + 2 * twos:2], tallies[2:2 + 2 * twos:2]
    slack = jnp.minimum(giver - 1, reach - sink)
    shifted = jax.random.randint(jax.random.fold_in(key, 1), (twos,), 0, 1 << 20) % (slack + 1)
    tallies = tallies.at[1:1 + 2 * twos:2].set(giver - shifted).at[2:2 + 2 * twos:2].set(sink + shifted)
    return tallies[jax.random.permutation(jax.random.fold_in(key, 2), amount)]


def noise(stream_key, dims, scale, most, pieces=(), kind=jnp.bfloat16):
    values = scale * jax.random.normal(stream_key, dims, jnp.float32)
    if pieces:
        values = values * shard_levels(stream_key, dims, pieces, -0.22, 0.18)
    return jnp.clip(values, -most, most).astype(kind)


def setup_inputs(seed: int = 0) -> dict:
    key_of = jax.random.split(jax.random.key(seed), 7)
    return {
        "queries": draw_queries(jax.random.fold_in(key_of[6], 71), 0),
        "keys": draw_keys(jax.random.fold_in(key_of[6], 71), 0),
        "values": noise(key_of[2], (TOKENS, D), 1.0, 6.0, ((0, 16), (1, 16))),
        "frame_of_block": jnp.searchsorted(jnp.cumsum(uneven_parts(key_of[3], FRAMES, NBLK, 4, 1)), jnp.arange(NBLK), side="right").astype(jnp.int32),
        "pair_mask": touch_ends((jax.random.randint(key_of[4], (NBLK, NBLK), 0, 4) < 3).astype(jnp.int32), jax.random.fold_in(key_of[4], 1), 0, 1),
        "w_out": noise(key_of[5], (D, D), (D // 32) ** -0.5, 0.4375, ((0, 16), (1, 16))),
    }


def reference(queries, keys, values, frame_of_block, pair_mask, w_out):
    width = H * HD
    scale = 1.0 / math.sqrt(HD)
    tok_frame = jnp.repeat(frame_of_block, BLK)
    key_block = (jnp.arange(TOKENS, dtype=jnp.int32) // BLK).astype(jnp.int32)
    count_blocks = TOKENS // TOK_DEV

    def one_block(index):
        first = (index * TOK_DEV).astype(jnp.int32)
        rows = lax.dynamic_slice_in_dim(queries, first, TOK_DEV, 0)
        q_frame = lax.dynamic_slice_in_dim(tok_frame, first, TOK_DEV, 0)
        q_block = ((first + jnp.arange(TOK_DEV, dtype=jnp.int32)) // BLK).astype(jnp.int32)
        link = pair_mask[q_block][:, key_block]
        allowed = (tok_frame[None, :] <= q_frame[:, None]) & ((link == 1) | (tok_frame[None, :] == q_frame[:, None]))

        def one_head(head_index):
            col = (head_index * HD).astype(jnp.int32)
            q_head = lax.dynamic_slice_in_dim(rows, col, HD, 1)
            k_head = lax.dynamic_slice_in_dim(keys, col, HD, 1)
            v_head = lax.dynamic_slice_in_dim(values, col, HD, 1)
            score = jnp.dot(q_head, k_head.T, preferred_element_type=jnp.float32) * scale
            score = jnp.where(allowed, score, -1e+30)
            peak = lax.optimization_barrier(jnp.max(score, axis=1))
            weight = jnp.where(allowed, jnp.exp(score - peak[:, None]), 0.0)
            total = lax.optimization_barrier(jnp.sum(weight, axis=1))
            mixed = jnp.dot(weight.astype(jnp.bfloat16), v_head, preferred_element_type=jnp.float32)
            return mixed / total[:, None]
        heads = lax.map(one_head, jnp.arange(H, dtype=jnp.int32))
        return jnp.transpose(heads, (1, 0, 2)).reshape(TOK_DEV, width).astype(jnp.bfloat16)
    attn = lax.map(one_block, jnp.arange(count_blocks, dtype=jnp.int32)).reshape(TOKENS, width)
    return jnp.dot(attn, w_out, preferred_element_type=jnp.float32).astype(jnp.bfloat16)
```

```python
import functools
import math

import jax
import jax.numpy as jnp
from jax import lax
from jax.experimental import pallas as pl
from jax.experimental.pallas import tpu as pltpu
from jax.sharding import PartitionSpec as P

HD = 128
BLK = 256
MESH = pl.DeviceIdType.MESH
ANY = pl.ANY


def where_am_i():
    s, h = lax.axis_index("seq"), lax.axis_index("head")
    c = lax.rem(h, 2)
    return s, h - c, c, s // 2, lax.rem(s, 2)


def worker_of(s):
    low = lax.rem(s, 8)
    return jnp.where(low < 4, low, 7 - low)


def chunk_owner(kk, j):
    return (kk, 7 - kk, 8 + kk, 15 - kk)[j]


def remote(src, dst, send, recv, seq, head):
    return pltpu.make_async_remote_copy(
        src_ref=src, dst_ref=dst, send_sem=send, recv_sem=recv, device_id=(seq, head), device_id_type=MESH
    )


def spread_kernel(q, k, v, meta, qb, kv, mt, s_kv, s_q, s_m, s_f, r_z, r_x, r_s, r_q, r_m):
    s, hb, c, z, x = where_am_i()
    barrier = pltpu.get_barrier_semaphore()

    def greet(n, _):
        ps, pc = n // 2, lax.rem(n, 2)

        @pl.when(jnp.logical_not((ps == s) & (pc == c)))
        def _():
            pl.semaphore_signal(barrier, inc=1, device_id=(ps, hb + pc), device_id_type=MESH)

        return 0

    lax.fori_loop(0, 32, greet, 0)
    pl.semaphore_wait(barrier, 31)

    def put(src, dst, send, recv, seq, head, start):
        mine = (seq == s) & (head == hb + c)
        copy = remote(src, dst, send, recv, seq, head)
        if start:

            @pl.when(mine)
            def _():
                pltpu.make_async_copy(src, dst, recv).start()

            @pl.when(jnp.logical_not(mine))
            def _():
                copy.start()
        else:

            @pl.when(jnp.logical_not(mine))
            def _():
                copy.wait_send()

    def all_sends(start):
        for i in range(3):
            pz = 4 * c + i
            cols = pl.ds(i * HD, HD)
            for t, src in ((0, k), (1, v)):
                put(src.at[:, cols], kv.at[t, s], s_kv.at[i, t], r_z.at[z], 2 * pz + x, hb + t, start)
        kk = worker_of(s)
        for i in range(3):
            pz = 4 * c + i
            cols = pl.ds(i * HD, HD)
            put(q.at[:, cols], qb.at[s // 4], s_q.at[i], r_q.at[s // 4], 2 * pz + lax.rem(kk, 2), hb + kk // 2, start)
            for px in range(2):
                for pc in range(2):
                    put(meta, mt.at[s], s_m.at[i, px, pc], r_m, 2 * pz + px, hb + pc, start)

    all_sends(True)

    def source_at(n):
        far = (n + 1) // 2
        return lax.rem(z + jnp.where(lax.rem(n, 2) == 1, far, 8 - far), 8)

    def to_sibling(piece):
        return remote(kv.at[c, piece], kv.at[c, piece], s_f.at[0, piece], r_s.at[piece], s, hb + 1 - c)

    def to_partner(zs):
        piece = 2 * zs + x
        return remote(kv.at[c, piece], kv.at[c, piece], s_f.at[1, zs], r_x.at[zs], 2 * z + 1 - x, hb + c)

    @pl.when(lax.rem(z, 4) < 3)
    def _():
        def turn(n, _):
            @pl.when(n < 8)
            def _():
                zs = source_at(n)
                piece = 2 * zs + x
                pltpu.make_async_copy(kv.at[c, piece], kv.at[c, piece], r_z.at[zs]).wait()
                to_partner(zs).start()
                to_sibling(piece).start()

            @pl.when(n > 0)
            def _():
                zs = source_at(n - 1)
                piece = 2 * zs + 1 - x
                pltpu.make_async_copy(kv.at[c, piece], kv.at[c, piece], r_x.at[zs]).wait()
                to_sibling(piece).start()

            return 0

        lax.fori_loop(0, 9, turn, 0)
        for j in range(4):
            pltpu.make_async_copy(qb.at[j], qb.at[j], r_q.at[j]).wait()
        pltpu.make_async_copy(mt, mt, r_m).wait()

        def settle(n, _):
            pltpu.make_async_copy(kv.at[1 - c, n], kv.at[1 - c, n], r_s.at[n]).wait()
            to_sibling(n).wait_send()
            return 0

        lax.fori_loop(0, 16, settle, 0)

        def sent(n, _):
            to_partner(n).wait_send()
            return 0

        lax.fori_loop(0, 8, sent, 0)

    all_sends(False)


def spread(q, k, v, meta):
    dma = pltpu.SemaphoreType.DMA
    tok = q.shape[0]
    return pl.pallas_call(
        spread_kernel,
        name="spread",
        out_shape=(
            jax.ShapeDtypeStruct((4, tok, HD), q.dtype),
            jax.ShapeDtypeStruct((2, 16, tok, HD), q.dtype),
            jax.ShapeDtypeStruct((16, 1, 128), jnp.int32),
        ),
        in_specs=[pl.BlockSpec(memory_space=ANY)] * 4,
        out_specs=[pl.BlockSpec(memory_space=ANY)] * 3,
        scratch_shapes=[
            dma((3, 2)), dma((3,)), dma((3, 2, 2)), dma((2, 16)),
            dma((8,)), dma((8,)), dma((16,)), dma((4,)), dma,
        ],
        compiler_params=pltpu.CompilerParams(collective_id=0, has_side_effects=True),
    )(q, k, v, meta)


GROUP = 4


def attend_kernel(meta, q_ref, kv_ref, o_ref, table, vext, acc, peak):
    s, hb, c, z, x = where_am_i()
    kk = 2 * c + x
    factor = math.log2(math.e) / math.sqrt(HD)

    @pl.when(lax.rem(z, 4) < 3)
    def _():
        def widen(n, _):
            vext[n, :, :HD] = kv_ref[1, n]
            vext[n, :, HD:] = jnp.ones((2 * BLK, HD), jnp.bfloat16)
            return 0

        lax.fori_loop(0, 16, widen, 0)

        def one_block(b, _):
            j, half = b // 2, lax.rem(b, 2)
            owner = jnp.where(
                j == 0, kk, jnp.where(j == 1, 7 - kk, jnp.where(j == 2, 8 + kk, 15 - kk))
            )
            row = 2 * owner + half
            frame = meta[owner, 0, 64 + half]

            def scan(d, count):
                for e in range(2):
                    near = meta[owner, 0, half * 32 + 2 * d + e] == 1
                    same = meta[d, 0, 64 + e] == frame
                    ok = ((2 * d + e <= row) & near) | same
                    table[count] = 2 * d + e
                    count = count + ok.astype(jnp.int32)
                return count

            count = lax.fori_loop(0, jnp.minimum(16, owner + 3), scan, 0)
            rows = pl.ds(pl.multiple_of(half * BLK, BLK), BLK)
            q = q_ref[j, rows, :]
            acc[...] = jnp.zeros_like(acc)
            peak[...] = jnp.full_like(peak, -1e30)

            def step(first, many):
                scores = []
                values = []
                for u in range(many):
                    blk = table[first + u]
                    krows = pl.ds(pl.multiple_of(lax.rem(blk, 2) * BLK, BLK), BLK)
                    keys = kv_ref[0, blk // 2, krows, :]
                    values.append((blk // 2, krows))
                    scores.append(
                        lax.dot_general(q, keys, (((1,), (1,)), ((), ())), preferred_element_type=jnp.float32)
                    )
                top = scores[0]
                for more in scores[1:]:
                    top = jnp.maximum(top, more)
                old = peak[...]
                new = jnp.maximum(old, jnp.max(top, axis=1, keepdims=True))
                peak[...] = new
                shrink = jnp.exp2((old - new) * factor)
                added = None
                for u in range(many):
                    weight = jnp.exp2((scores[u] - new[:, :1]) * factor).astype(jnp.bfloat16)
                    part = jnp.dot(
                        weight, vext[values[u][0], values[u][1], :], preferred_element_type=jnp.float32
                    )
                    added = part if added is None else added + part
                acc[:, :HD] = acc[:, :HD] * shrink + added[:, :HD]
                acc[:, HD:] = acc[:, HD:] * shrink + added[:, HD:]

            whole = count // GROUP

            def group(g, _):
                step(g * GROUP, GROUP)
                return 0

            lax.fori_loop(0, whole, group, 0)

            def single(g, _):
                step(g, 1)
                return 0

            lax.fori_loop(whole * GROUP, count, single, 0)
            o_ref[j, rows, :] = (acc[:, :HD] / acc[:, HD:]).astype(jnp.bfloat16)
            return 0

        lax.fori_loop(0, 8, one_block, 0)


def attend(meta, q, kv):
    return pl.pallas_call(
        attend_kernel,
        name="attend",
        out_shape=jax.ShapeDtypeStruct(q.shape, q.dtype),
        in_specs=[
            pl.BlockSpec(memory_space=pltpu.SMEM),
            pl.BlockSpec(memory_space=pltpu.VMEM),
            pl.BlockSpec(memory_space=pltpu.VMEM),
        ],
        out_specs=pl.BlockSpec(memory_space=pltpu.VMEM),
        scratch_shapes=[
            pltpu.SMEM((36,), jnp.int32),
            pltpu.VMEM((16, 2 * BLK, 2 * HD), jnp.bfloat16),
            pltpu.VMEM((BLK, 2 * HD), jnp.float32),
            pltpu.VMEM((BLK, HD), jnp.float32),
        ],
        cost_estimate=pl.CostEstimate(flops=20_000_000_000, bytes_accessed=8_000_000, transcendentals=0),
    )(meta, q, kv)


def collect_kernel(o, attn, send, recv):
    s, hb, c, z, x = where_am_i()
    kk = 2 * c + x
    barrier = pltpu.get_barrier_semaphore()
    w = worker_of(s)
    for i in range(3):
        ps, ph = 2 * (4 * c + i) + lax.rem(w, 2), hb + w // 2

        @pl.when(jnp.logical_not((ps == s) & (ph == hb + c)))
        def _():
            pl.semaphore_signal(barrier, inc=1, device_id=(ps, ph), device_id_type=MESH)

    i = lax.rem(z, 4)
    to_head = hb + z // 4
    cols = pl.ds(pl.multiple_of(i * HD, HD), HD)

    def each(fn):
        for j in range(4):
            to = chunk_owner(kk, j)
            mine = (to == s) & (to_head == hb + c)
            fn(j, to, mine)

    @pl.when(i < 3)
    def _():
        own = sum(((chunk_owner(kk, j) == s) & (to_head == hb + c)).astype(jnp.int32) for j in range(4))
        pl.semaphore_wait(barrier, 4 - own)

        def begin(j, to, mine):
            @pl.when(mine)
            def _():
                pltpu.make_async_copy(o.at[j], attn.at[:, cols], recv.at[i]).start()

            @pl.when(jnp.logical_not(mine))
            def _():
                remote(o.at[j], attn.at[:, cols], send.at[j], recv.at[i], to, to_head).start()

        each(begin)

    for n in range(3):
        got = attn.at[:, pl.ds(n * HD, HD)]
        pltpu.make_async_copy(got, got, recv.at[n]).wait()

    @pl.when(i < 3)
    def _():
        def sent(j, to, mine):
            @pl.when(jnp.logical_not(mine))
            def _():
                remote(o.at[j], attn.at[:, cols], send.at[j], recv.at[i], to, to_head).wait_send()

        each(sent)


def collect(o):
    tok = o.shape[1]
    return pl.pallas_call(
        collect_kernel,
        name="collect",
        out_shape=jax.ShapeDtypeStruct((tok, 3 * HD), o.dtype),
        in_specs=[pl.BlockSpec(memory_space=ANY)],
        out_specs=pl.BlockSpec(memory_space=ANY),
        scratch_shapes=[pltpu.SemaphoreType.DMA((4,)), pltpu.SemaphoreType.DMA((3,))],
        compiler_params=pltpu.CompilerParams(collective_id=1, has_side_effects=True),
    )(o)


def body(queries, keys, values, frame_of_block, pair_mask, w_out):
    turned = lax.ppermute(
        w_out, ("seq", "head"), [(a * 16 + b, b * 16 + a) for a in range(16) for b in range(16)]
    )
    columns = lax.all_gather(turned, "seq", axis=0, tiled=True)
    meta = jnp.concatenate(
        [pair_mask.reshape(-1), frame_of_block, jnp.zeros((62,), jnp.int32)]
    ).reshape(1, 128)
    qb, kv, mt = spread(queries, keys, values, meta)
    o = attend(mt, qb, kv)
    attn = collect(o)
    full_attn = lax.all_gather(attn, "head", axis=1, tiled=True)
    return jnp.dot(full_attn, columns, preferred_element_type=jnp.float32).astype(jnp.bfloat16)


def solution(mesh):
    return jax.shard_map(
        body,
        mesh=mesh,
        in_specs=(
            P("seq", "head"),
            P("seq", "head"),
            P("seq", "head"),
            P("seq"),
            P("seq", None),
            P("head", "seq"),
        ),
        out_specs=P("seq", "head"),
        check_vma=False,
    )
```

```python
import functools
import math

import jax
import jax.numpy as jnp
from jax import lax
from jax.experimental import pallas as pl
from jax.experimental.pallas import tpu as pltpu
from jax.sharding import PartitionSpec as P

HD = 128
BLK = 256
MESH = pl.DeviceIdType.MESH
ANY = pl.ANY


def where_am_i():
    s, h = lax.axis_index("seq"), lax.axis_index("head")
    c = lax.rem(h, 2)
    return s, h - c, c, s // 2, lax.rem(s, 2)


def worker_of(s):
    low = lax.rem(s, 8)
    return jnp.where(low < 4, low, 7 - low)


def chunk_owner(kk, j):
    return (kk, 7 - kk, 8 + kk, 15 - kk)[j]


def remote(src, dst, send, recv, seq, head):
    return pltpu.make_async_remote_copy(
        src_ref=src, dst_ref=dst, send_sem=send, recv_sem=recv, device_id=(seq, head), device_id_type=MESH
    )


def spread_kernel(q, k, v, meta, w, qb, kv, mt, wb, s_kv, s_q, s_m, s_f, s_w, r_z, r_x, r_s, r_q, r_m, r_w):
    s, hb, c, z, x = where_am_i()
    y, x_hi = hb // 4, lax.rem(hb, 4) // 2
    barrier = pltpu.get_barrier_semaphore()

    def greet(n, _):
        ps, pc = n // 2, lax.rem(n, 2)

        @pl.when(jnp.logical_not((ps == s) & (pc == c)))
        def _():
            pl.semaphore_signal(barrier, inc=1, device_id=(ps, hb + pc), device_id_type=MESH)

        return 0

    lax.fori_loop(0, 32, greet, 0)

    def greet_row(n, _):
        other = 4 * y + 2 * (1 - x_hi) + n
        pl.semaphore_signal(barrier, inc=1, device_id=(s, other), device_id_type=MESH)
        return 0

    lax.fori_loop(0, 2, greet_row, 0)
    pl.semaphore_wait(barrier, 33)

    def put(src, dst, send, recv, seq, head, start):
        mine = (seq == s) & (head == hb + c)
        copy = remote(src, dst, send, recv, seq, head)
        if start:

            @pl.when(mine)
            def _():
                pltpu.make_async_copy(src, dst, recv).start()

            @pl.when(jnp.logical_not(mine))
            def _():
                copy.start()
        else:

            @pl.when(jnp.logical_not(mine))
            def _():
                copy.wait_send()

    def all_sends(start):
        here = wb.at[lax.rem(z, 4) // 2, 2 * x_hi + c]
        put(
            w, here, s_w.at[2, 0, 0], r_w.at[lax.rem(z, 4) // 2, 2 * x_hi + c],
            s, 4 * y + 2 * lax.rem(z, 2) + z // 4, start,
        )
        for i in range(3):
            pz = 4 * c + i
            cols = pl.ds(i * HD, HD)
            for t, src in ((0, k), (1, v)):
                put(src.at[:, cols], kv.at[t, s], s_kv.at[i, t], r_z.at[z], 2 * pz + x, hb + t, start)
        kk = worker_of(s)
        for i in range(3):
            pz = 4 * c + i
            cols = pl.ds(i * HD, HD)
            put(q.at[:, cols], qb.at[s // 4], s_q.at[i], r_q.at[s // 4], 2 * pz + lax.rem(kk, 2), hb + kk // 2, start)
            for px in range(2):
                for pc in range(2):
                    put(meta, mt.at[s], s_m.at[i, px, pc], r_m, 2 * pz + px, hb + pc, start)

    all_sends(True)

    def source_at(n):
        far = (n + 1) // 2
        return lax.rem(z + jnp.where(lax.rem(n, 2) == 1, far, 8 - far), 8)

    def to_sibling(piece):
        return remote(kv.at[c, piece], kv.at[c, piece], s_f.at[0, piece], r_s.at[piece], s, hb + 1 - c)

    def to_partner(zs):
        piece = 2 * zs + x
        return remote(kv.at[c, piece], kv.at[c, piece], s_f.at[1, zs], r_x.at[zs], 2 * z + 1 - x, hb + c)

    def w_hop(e, r, up):
        piece = wb.at[e, r]
        to = lax.rem(z + (1 if up else 7), 8)
        return remote(piece, piece, s_w.at[1 if up else 0, e, r], r_w.at[e, r], 2 * to + x, hb + c)

    def w_far(e):
        return lax.rem(z - (4 * c + 2 * e + x_hi) + 8, 8)

    def w_turn(n):
        for e in range(2):
            far = w_far(e)
            r = n - jnp.where(far > 4, 8 - far, far)

            @pl.when((r >= 0) & (r < 4))
            def _():
                pltpu.make_async_copy(wb.at[e, r], wb.at[e, r], r_w.at[e, r]).wait()

                @pl.when(far < 4)
                def _():
                    w_hop(e, r, True).start()

                @pl.when((far == 0) | (far > 5))
                def _():
                    w_hop(e, r, False).start()

    def w_sent(r, _):
        for e in range(2):
            far = w_far(e)

            @pl.when(far < 4)
            def _():
                w_hop(e, r, True).wait_send()

            @pl.when((far == 0) | (far > 5))
            def _():
                w_hop(e, r, False).wait_send()

        return 0

    working = lax.rem(z, 4) < 3

    def turn(n, _):
        @pl.when(working)
        def _():
            @pl.when(n < 8)
            def _():
                zs = source_at(n)
                piece = 2 * zs + x
                pltpu.make_async_copy(kv.at[c, piece], kv.at[c, piece], r_z.at[zs]).wait()
                to_partner(zs).start()
                to_sibling(piece).start()

            @pl.when(n > 0)
            def _():
                zs = source_at(n - 1)
                piece = 2 * zs + 1 - x
                pltpu.make_async_copy(kv.at[c, piece], kv.at[c, piece], r_x.at[zs]).wait()
                to_sibling(piece).start()

        w_turn(n)
        return 0

    lax.fori_loop(0, 9, turn, 0)

    @pl.when(working)
    def _():
        for j in range(4):
            pltpu.make_async_copy(qb.at[j], qb.at[j], r_q.at[j]).wait()
        pltpu.make_async_copy(mt, mt, r_m).wait()

        def settle(n, _):
            pltpu.make_async_copy(kv.at[1 - c, n], kv.at[1 - c, n], r_s.at[n]).wait()
            to_sibling(n).wait_send()
            return 0

        lax.fori_loop(0, 16, settle, 0)

        def sent(n, _):
            to_partner(n).wait_send()
            return 0

        lax.fori_loop(0, 8, sent, 0)

    lax.fori_loop(0, 4, w_sent, 0)
    all_sends(False)


def spread(q, k, v, meta, w):
    dma = pltpu.SemaphoreType.DMA
    tok = q.shape[0]
    return pl.pallas_call(
        spread_kernel,
        name="spread",
        out_shape=(
            jax.ShapeDtypeStruct((4, tok, HD), q.dtype),
            jax.ShapeDtypeStruct((2, 16, tok, HD), q.dtype),
            jax.ShapeDtypeStruct((16, 1, 128), jnp.int32),
            jax.ShapeDtypeStruct((2, 4) + w.shape, w.dtype),
        ),
        in_specs=[pl.BlockSpec(memory_space=ANY)] * 5,
        out_specs=[pl.BlockSpec(memory_space=ANY)] * 4,
        scratch_shapes=[
            dma((3, 2)), dma((3,)), dma((3, 2, 2)), dma((2, 16)), dma((3, 2, 4)),
            dma((8,)), dma((8,)), dma((16,)), dma((4,)), dma, dma((2, 4)),
        ],
        compiler_params=pltpu.CompilerParams(collective_id=0, has_side_effects=True),
    )(q, k, v, meta, w)


GROUP = 4


def attend_kernel(meta, q_ref, kv_ref, o_ref, table, vext, acc, peak):
    s, hb, c, z, x = where_am_i()
    kk = 2 * c + x
    factor = math.log2(math.e) / math.sqrt(HD)

    @pl.when(lax.rem(z, 4) < 3)
    def _():
        def widen(n, _):
            vext[n, :, :HD] = kv_ref[1, n]
            vext[n, :, HD:] = jnp.ones((2 * BLK, HD), jnp.bfloat16)
            return 0

        lax.fori_loop(0, 16, widen, 0)

        def one_block(b, _):
            j, half = b // 2, lax.rem(b, 2)
            owner = jnp.where(
                j == 0, kk, jnp.where(j == 1, 7 - kk, jnp.where(j == 2, 8 + kk, 15 - kk))
            )
            row = 2 * owner + half
            frame = meta[owner, 0, 64 + half]

            def scan(d, count):
                for e in range(2):
                    near = meta[owner, 0, half * 32 + 2 * d + e] == 1
                    same = meta[d, 0, 64 + e] == frame
                    ok = ((2 * d + e <= row) & near) | same
                    table[count] = 2 * d + e
                    count = count + ok.astype(jnp.int32)
                return count

            count = lax.fori_loop(0, jnp.minimum(16, owner + 3), scan, 0)
            rows = pl.ds(pl.multiple_of(half * BLK, BLK), BLK)
            q = q_ref[j, rows, :]
            acc[...] = jnp.zeros_like(acc)
            peak[...] = jnp.full_like(peak, -1e30)

            def step(first, many):
                scores = []
                values = []
                for u in range(many):
                    blk = table[first + u]
                    krows = pl.ds(pl.multiple_of(lax.rem(blk, 2) * BLK, BLK), BLK)
                    keys = kv_ref[0, blk // 2, krows, :]
                    values.append((blk // 2, krows))
                    scores.append(
                        lax.dot_general(q, keys, (((1,), (1,)), ((), ())), preferred_element_type=jnp.float32)
                    )
                top = scores[0]
                for more in scores[1:]:
                    top = jnp.maximum(top, more)
                old = peak[...]
                new = jnp.maximum(old, jnp.max(top, axis=1, keepdims=True))
                peak[...] = new
                shrink = jnp.exp2((old - new) * factor)
                added = None
                for u in range(many):
                    weight = jnp.exp2((scores[u] - new[:, :1]) * factor).astype(jnp.bfloat16)
                    part = jnp.dot(
                        weight, vext[values[u][0], values[u][1], :], preferred_element_type=jnp.float32
                    )
                    added = part if added is None else added + part
                acc[:, :HD] = acc[:, :HD] * shrink + added[:, :HD]
                acc[:, HD:] = acc[:, HD:] * shrink + added[:, HD:]

            whole = count // GROUP

            def group(g, _):
                step(g * GROUP, GROUP)
                return 0

            lax.fori_loop(0, whole, group, 0)

            def single(g, _):
                step(g, 1)
                return 0

            lax.fori_loop(whole * GROUP, count, single, 0)
            o_ref[j, rows, :] = (acc[:, :HD] / acc[:, HD:]).astype(jnp.bfloat16)
            return 0

        lax.fori_loop(0, 8, one_block, 0)


def attend(meta, q, kv):
    return pl.pallas_call(
        attend_kernel,
        name="attend",
        out_shape=jax.ShapeDtypeStruct(q.shape, q.dtype),
        in_specs=[
            pl.BlockSpec(memory_space=pltpu.SMEM),
            pl.BlockSpec(memory_space=pltpu.VMEM),
            pl.BlockSpec(memory_space=pltpu.VMEM),
        ],
        out_specs=pl.BlockSpec(memory_space=pltpu.VMEM),
        scratch_shapes=[
            pltpu.SMEM((36,), jnp.int32),
            pltpu.VMEM((16, 2 * BLK, 2 * HD), jnp.bfloat16),
            pltpu.VMEM((BLK, 2 * HD), jnp.float32),
            pltpu.VMEM((BLK, HD), jnp.float32),
        ],
        cost_estimate=pl.CostEstimate(flops=20_000_000_000, bytes_accessed=8_000_000, transcendentals=0),
    )(meta, q, kv)


def project_kernel(o, w, out, a, part, got, s_o, s_x, s_s, s_p, r_o, r_x, r_s, r_p):
    s, hb, c, z, x_lo = where_am_i()
    y, x_hi = hb // 4, lax.rem(hb, 4) // 2
    x = 2 * x_hi + x_lo
    kk = 2 * c + x_lo
    barrier = pltpu.get_barrier_semaphore()

    def greet(seq, head):
        pl.semaphore_signal(barrier, inc=1, device_id=(seq, head), device_id_type=MESH)

    def greet_group(n, _):
        ps, pc = n // 2, lax.rem(n, 2)

        @pl.when(jnp.logical_not((ps == s) & (pc == c)))
        def _():
            greet(ps, hb + pc)

        return 0

    def greet_row(n, _):
        greet(2 * z + n // 2, 4 * y + 2 * (1 - x_hi) + lax.rem(n, 2))
        return 0

    def greet_line(n, _):
        py = lax.rem(y + 1 + n // 4, 4)
        greet(2 * z + lax.rem(n, 4) // 2, 4 * py + 2 * x_hi + lax.rem(n, 2))
        return 0

    lax.fori_loop(0, 32, greet_group, 0)
    lax.fori_loop(0, 4, greet_row, 0)
    lax.fori_loop(0, 12, greet_line, 0)
    pl.semaphore_wait(barrier, 47)

    def move(src, dst, send, recv, seq, head, start):
        mine = (seq == s) & (head == hb + c)
        copy = remote(src, dst, send, recv, seq, head)
        if start:

            @pl.when(mine)
            def _():
                pltpu.make_async_copy(src, dst, recv).start()

            @pl.when(jnp.logical_not(mine))
            def _():
                copy.start()
        else:

            @pl.when(jnp.logical_not(mine))
            def _():
                copy.wait_send()

    def arrived(ref, sem):
        pltpu.make_async_copy(ref, ref, sem).wait()

    def cols(i):
        return pl.ds(i * HD, HD)

    third = lax.rem(z, 4)

    def give_back(start):
        @pl.when(third < 3)
        def _():
            lanes = pl.ds(pl.multiple_of(third * HD, HD), HD)
            for j in range(4):
                to = chunk_owner(kk, j)
                slot = 2 * x_hi + lax.rem(to, 2)
                move(o.at[j], a.at[slot, z // 4, :, lanes], s_o.at[j], r_o.at[third], to, hb + z // 4, start)

    def to_sibling(slot, i):
        piece = a.at[slot, c, :, cols(i)]
        return remote(piece, piece, s_s.at[slot, i], r_s.at[slot, i], s, hb + 1 - c)

    def to_row(dx, i):
        px = lax.rem(x + dx, 4)
        piece = a.at[x, c, :, cols(i)]
        return remote(piece, piece, s_x.at[dx, i], r_x.at[x, i], 2 * z + lax.rem(px, 2), 4 * y + 2 * (px // 2) + c)

    give_back(True)
    for i in range(3):
        arrived(a.at[x, c, :, cols(i)], r_o.at[i])
        for dx in (1, 3, 2):
            to_row(dx, i).start()
        to_sibling(x, i).start()
    for i in range(3):
        for dx in (3, 1, 2):
            slot = lax.rem(x + dx, 4)
            arrived(a.at[slot, c, :, cols(i)], r_x.at[slot, i])
            to_sibling(slot, i).start()
    for slot in range(4):
        for i in range(3):
            arrived(a.at[slot, 1 - c, :, cols(i)], r_s.at[slot, i])

    def pass_on(t, e, start):
        py = 2 * c + e
        move(part.at[t, e], got.at[y], s_p.at[t, e], r_p.at[y], 2 * z + t, 4 * py + 2 * x_hi + x_lo, start)

    for t in range(2):
        for e in range(2):

            def tile(n, _):
                rows = pl.ds(pl.multiple_of(n * 128, 128), 128)
                total = None
                for r in range(4):
                    dot = jnp.dot(
                        a[2 * (r // 2) + t, r % 2, rows, :], w[e, r], preferred_element_type=jnp.float32
                    )
                    total = dot if total is None else total + dot
                part[t, e, rows, :] = total.astype(jnp.bfloat16)
                return 0

            lax.fori_loop(0, 4, tile, 0)
            pass_on(t, e, True)
    for n in range(4):
        arrived(got.at[n], r_p.at[n])

    def add(n, _):
        rows = pl.ds(pl.multiple_of(n * 64, 64), 64)
        total = got[0, rows, :].astype(jnp.float32)
        for m in range(1, 4):
            total = total + got[m, rows, :].astype(jnp.float32)
        out[rows, :] = total.astype(jnp.bfloat16)
        return 0

    lax.fori_loop(0, 8, add, 0)
    give_back(False)
    for i in range(3):
        for dx in (1, 2, 3):
            to_row(dx, i).wait_send()
        for slot in range(4):
            to_sibling(slot, i).wait_send()
    for t in range(2):
        for e in range(2):
            pass_on(t, e, False)


def project(o, w):
    dma = pltpu.SemaphoreType.DMA
    tok = o.shape[1]
    wide = 3 * HD
    return pl.pallas_call(
        project_kernel,
        name="project",
        out_shape=jax.ShapeDtypeStruct((tok, wide), o.dtype),
        in_specs=[pl.BlockSpec(memory_space=pltpu.VMEM)] * 2,
        out_specs=pl.BlockSpec(memory_space=pltpu.VMEM),
        scratch_shapes=[
            pltpu.VMEM((4, 2, tok, wide), jnp.bfloat16),
            pltpu.VMEM((2, 2, tok, wide), jnp.bfloat16),
            pltpu.VMEM((4, tok, wide), jnp.bfloat16),
            dma((4,)), dma((4, 3)), dma((4, 3)), dma((2, 2)),
            dma((3,)), dma((4, 3)), dma((4, 3)), dma((4,)),
        ],
        compiler_params=pltpu.CompilerParams(collective_id=1, has_side_effects=True),
    )(o, w)


def body(queries, keys, values, frame_of_block, pair_mask, w_out):
    meta = jnp.concatenate(
        [pair_mask.reshape(-1), frame_of_block, jnp.zeros((62,), jnp.int32)]
    ).reshape(1, 128)
    qb, kv, mt, wb = spread(queries, keys, values, meta, w_out)
    return project(attend(mt, qb, kv), wb)


def solution(mesh):
    return jax.shard_map(
        body,
        mesh=mesh,
        in_specs=(
            P("seq", "head"),
            P("seq", "head"),
            P("seq", "head"),
            P("seq"),
            P("seq", None),
            P("head", "seq"),
        ),
        out_specs=P("seq", "head"),
        check_vma=False,
    )
```

```python
import math

import jax
import jax.numpy as jnp
from jax import lax
from jax.experimental import pallas as pl
from jax.experimental.pallas import tpu as pltpu
from jax.sharding import PartitionSpec as P

HD = 128
BLK = 256
TOK = 512
MESH = pl.DeviceIdType.MESH
VMEM = pltpu.VMEM
FACTOR = math.log2(math.e) / math.sqrt(HD)


def remote(src, dst, send, recv, seq, head):
    return pltpu.make_async_remote_copy(
        src_ref=src, dst_ref=dst, send_sem=send, recv_sem=recv, device_id=(seq, head), device_id_type=MESH
    )


def arrived(ref, sem):
    pltpu.make_async_copy(ref, ref, sem).wait()


def chunk_owner(kk, j):
    return jnp.where(j == 0, kk, jnp.where(j == 1, 7 - kk, jnp.where(j == 2, 8 + kk, 15 - kk)))


def kernel(
    q, k, v, meta, w, out,
    qb, kv, mt, table, wb, acc, peak, ob, a, part, got,
    s_q, s_kv, s_m, s_f, s_p, s_w, r_q, r_z, r_x, r_s, r_m, r_w, r_t,
    s_o, s_a, s_b, s_d, r_o, r_a, r_b, r_d,
):
    s, h = lax.axis_index("seq"), lax.axis_index("head")
    c = lax.rem(h, 2)
    hb = h - c
    z, x_lo = s // 2, lax.rem(s, 2)
    y, x_hi = hb // 4, lax.rem(hb, 4) // 2
    x = 2 * x_hi + x_lo
    kk = 2 * c + x_lo
    third = lax.rem(z, 4)
    working = third < 3
    barrier = pltpu.get_barrier_semaphore()

    def greet(seq, head):
        pl.semaphore_signal(barrier, inc=1, device_id=(seq, head), device_id_type=MESH)

    def greet_group(n, _):
        ps, pc = n // 2, lax.rem(n, 2)

        @pl.when(jnp.logical_not((ps == s) & (pc == c)))
        def _():
            greet(ps, hb + pc)

        return 0

    def greet_row(n, _):
        greet(2 * z + n // 2, 4 * y + 2 * (1 - x_hi) + lax.rem(n, 2))
        return 0

    def greet_line(n, _):
        py = lax.rem(y + 1 + n // 4, 4)
        greet(2 * z + lax.rem(n, 4) // 2, 4 * py + 2 * x_hi + lax.rem(n, 2))
        return 0

    lax.fori_loop(0, 32, greet_group, 0)
    lax.fori_loop(0, 4, greet_row, 0)
    lax.fori_loop(0, 12, greet_line, 0)
    pl.semaphore_wait(barrier, 47)

    def put(src, dst, send, recv, seq, head, start):
        mine = (seq == s) & (head == h)
        copy = remote(src, dst, send, recv, seq, head)
        if start:

            @pl.when(mine)
            def _():
                pltpu.make_async_copy(src, dst, recv).start()

            @pl.when(jnp.logical_not(mine))
            def _():
                copy.start()
        else:

            @pl.when(jnp.logical_not(mine))
            def _():
                copy.wait_send()

    def cols(i):
        return pl.ds(i * HD, HD)

    rising = lax.rem(z - 4 * c + 9, 8) < 2
    low = lax.rem(s, 8)
    worker = jnp.where(low < 4, low, 7 - low)

    def spread(start):
        for r in range(3):
            i = jnp.where(rising | (z == 4 * c + 6 - 8 * c), r, 2 - r)
            pz = 4 * c + i
            lanes = pl.ds(pl.multiple_of(i * HD, HD), HD)
            put(q.at[:, lanes], qb.at[s // 4], s_q.at[r], r_q.at[s // 4], 2 * pz + lax.rem(worker, 2), hb + worker // 2, start)
        for r in range(3):
            i = jnp.where(rising | (z == 4 * c + 6 - 8 * c), r, 2 - r)
            pz = 4 * c + i
            lanes = pl.ds(pl.multiple_of(i * HD, HD), HD)
            for px in range(2):
                for pc in range(2):
                    put(meta, mt.at[s], s_m.at[r, px, pc], r_m, 2 * pz + px, hb + pc, start)
            for t, src in ((0, k), (1, v)):
                put(src.at[:, lanes], kv.at[t, s], s_kv.at[r, t], r_z.at[z], 2 * pz + x_lo, hb + t, start)
        e, r = lax.rem(z, 4) // 2, 2 * x_hi + c
        put(w, wb.at[e, r], s_w.at[2, 0, 0], r_w.at[e, r], s, 4 * y + 2 * lax.rem(z, 2) + z // 4, start)

    spread(True)

    def source_at(n):
        far = (n + 1) // 2
        return lax.rem(z + jnp.where(lax.rem(n, 2) == 1, far, 8 - far), 8)

    def to_sibling(piece):
        return remote(kv.at[c, piece], kv.at[c, piece], s_f.at[piece], r_s.at[piece], s, hb + 1 - c)

    def to_partner(zs):
        piece = 2 * zs + x_lo
        return remote(kv.at[c, piece], kv.at[c, piece], s_p.at[zs], r_x.at[zs], 2 * z + 1 - x_lo, h)

    def w_hop(e, r, up):
        to = lax.rem(z + (1 if up else 7), 8)
        return remote(wb.at[e, r], wb.at[e, r], s_w.at[1 if up else 0, e, r], r_w.at[e, r], 2 * to + x_lo, h)

    def w_far(e):
        return lax.rem(z - (4 * c + 2 * e + x_hi) + 8, 8)

    def w_turn(n):
        for e in range(2):
            far = w_far(e)
            r = n - jnp.where(far > 4, 8 - far, far)

            @pl.when((r >= 0) & (r < 4))
            def _():
                arrived(wb.at[e, r], r_w.at[e, r])

                @pl.when(far < 4)
                def _():
                    w_hop(e, r, True).start()

                @pl.when((far == 0) | (far > 5))
                def _():
                    w_hop(e, r, False).start()

    def w_sent(r, _):
        for e in range(2):
            far = w_far(e)

            @pl.when(far < 4)
            def _():
                w_hop(e, r, True).wait_send()

            @pl.when((far == 0) | (far > 5))
            def _():
                w_hop(e, r, False).wait_send()

        return 0

    def attend(piece, j, owner):
        keys = [kv[0, piece, pl.ds(u * BLK, BLK), :] for u in range(2)]
        ones = jnp.ones((BLK, HD), jnp.bfloat16)
        wide = [jnp.concatenate([kv[1, piece, pl.ds(u * BLK, BLK), :], ones], axis=1) for u in range(2)]
        for tile in range(4):
            half = tile // 2
            ok = []
            for u in range(2):
                near = (table[owner, 0, 32 * half + 2 * piece + u] == 1) & (2 * piece + u <= 2 * owner + half)
                ok.append(near | (table[piece, 0, 64 + u] == table[owner, 0, 64 + half]))
            rows = pl.ds(tile * 128, 128)
            held = pl.ds(pl.multiple_of(j * TOK + tile * 128, 128), 128)
            query = qb[j, rows, :]
            score = [
                lax.dot_general(query, keys[u], (((1,), (1,)), ((), ())), preferred_element_type=jnp.float32)
                for u in range(2)
            ]
            tops = [
                jnp.maximum(score[u][:, :HD], score[u][:, HD:]) + jnp.where(ok[u], 0.0, -1e30) for u in range(2)
            ]
            old = peak[held, :]
            new = jnp.maximum(old, jnp.max(jnp.maximum(tops[0], tops[1]), axis=1, keepdims=True))
            peak[held, :] = new
            shrink = jnp.exp2((old - new) * FACTOR)
            added = None
            for u in range(2):
                base = jnp.where(ok[u], new, 1e30)
                weight = jnp.concatenate(
                    [
                        jnp.exp2((score[u][:, cols_] - base) * FACTOR).astype(jnp.bfloat16)
                        for cols_ in (slice(0, HD), slice(HD, 2 * HD))
                    ],
                    axis=1,
                )
                dot = jnp.dot(weight, wide[u], preferred_element_type=jnp.float32)
                added = dot if added is None else added + dot
            acc[held, :HD] = acc[held, :HD] * shrink + added[:, :HD]
            acc[held, HD:] = acc[held, HD:] * shrink + added[:, HD:]

    @pl.when(working)
    def _():
        acc[...] = jnp.zeros_like(acc)
        peak[...] = jnp.full_like(peak, -1e30)

    def turn(n, _):
        @pl.when(working & (n < 8))
        def _():
            zs = source_at(n)
            piece = 2 * zs + x_lo
            arrived(kv.at[c, piece], r_z.at[zs])
            to_partner(zs).start()
            to_sibling(piece).start()

        @pl.when(working & (n > 0) & (n < 9))
        def _():
            zs = source_at(n - 1)
            piece = 2 * zs + 1 - x_lo
            arrived(kv.at[c, piece], r_x.at[zs])
            to_sibling(piece).start()

        @pl.when(n >= W_LAG)
        def _():
            w_turn(n - W_LAG)

        @pl.when(working & (n == 2))
        def _():
            for j in range(4):
                arrived(qb.at[j], r_q.at[j])
            arrived(mt, r_m)
            local = pltpu.make_async_copy(mt, table, r_t)
            local.start()
            local.wait()

        @pl.when(working & (n > 1) & (n < 10))
        def _():
            zs = source_at(n - 2)
            for side in range(2):
                piece = 2 * zs + side
                arrived(kv.at[1 - c, piece], r_s.at[piece])

            def one(m, _):
                piece, j = 2 * zs + m // 4, lax.rem(m, 4)
                owner = chunk_owner(kk, j)

                @pl.when(piece <= owner + 2)
                def _():
                    attend(piece, j, owner)

                return 0

            lax.fori_loop(0, 8, one, 0)

        return 0

    lax.fori_loop(0, max(10, 8 + W_LAG), turn, 0)

    def give_back(start):
        lanes = pl.ds(pl.multiple_of(third * HD, HD), HD)
        for j in range(4):
            to = chunk_owner(kk, j)
            slot = 2 * x_hi + lax.rem(to, 2)
            put(ob.at[j], a.at[slot, z // 4, :, lanes], s_o.at[j], r_o.at[third], to, hb + z // 4, start)

    @pl.when(working)
    def _():
        def finish(n, _):
            rows = pl.ds(pl.multiple_of(n * 128, 128), 128)
            ob[n // 4, pl.ds(pl.multiple_of(lax.rem(n, 4) * 128, 128), 128), :] = (
                acc[rows, :HD] / acc[rows, HD:]
            ).astype(jnp.bfloat16)
            return 0

        lax.fori_loop(0, 16, finish, 0)
        give_back(True)

    def cross(slot, i):
        piece = a.at[slot, c, :, cols(i)]
        return remote(piece, piece, s_b.at[slot, i], r_b.at[slot, i], s, hb + 1 - c)

    def to_row(dx, i):
        px = lax.rem(x + dx, 4)
        piece = a.at[x, c, :, cols(i)]
        return remote(piece, piece, s_a.at[dx, i], r_a.at[x, i], 2 * z + lax.rem(px, 2), 4 * y + 2 * (px // 2) + c)

    for i in range(3):
        arrived(a.at[x, c, :, cols(i)], r_o.at[i])
        for dx in (1, 3, 2):
            to_row(dx, i).start()
        cross(x, i).start()
    for i in range(3):
        for dx in (3, 1, 2):
            slot = lax.rem(x + dx, 4)
            arrived(a.at[slot, c, :, cols(i)], r_a.at[slot, i])
            cross(slot, i).start()
    for slot in range(4):
        for i in range(3):
            arrived(a.at[slot, 1 - c, :, cols(i)], r_b.at[slot, i])

    def pass_on(t, e, start):
        py = 2 * c + e
        put(part.at[t, e], got.at[y], s_d.at[t, e], r_d.at[y], 2 * z + t, 4 * py + 2 * x_hi + x_lo, start)

    before = None
    for t in range(2):
        for e in range(2):

            def tile(n, _):
                rows = pl.ds(pl.multiple_of(n * 128, 128), 128)
                total = None
                for r in range(4):
                    dot = jnp.dot(
                        a[2 * (r // 2) + t, r % 2, rows, :], wb[e, r], preferred_element_type=jnp.float32
                    )
                    total = dot if total is None else total + dot
                part[t, e, rows, :] = total.astype(jnp.bfloat16)
                return 0

            lax.fori_loop(0, 4, tile, 0)
            if before is not None:
                pass_on(*before, True)
            before = (t, e)
    pass_on(*before, True)
    for n in range(4):
        arrived(got.at[n], r_d.at[n])

    def add(n, _):
        rows = pl.ds(pl.multiple_of(n * 64, 64), 64)
        total = got[0, rows, :].astype(jnp.float32)
        for m in range(1, 4):
            total = total + got[m, rows, :].astype(jnp.float32)
        out[rows, :] = total.astype(jnp.bfloat16)
        return 0

    lax.fori_loop(0, 8, add, 0)

    spread(False)
    lax.fori_loop(0, 4, w_sent, 0)

    @pl.when(working)
    def _():
        def sent(n, _):
            to_sibling(2 * n).wait_send()
            to_sibling(2 * n + 1).wait_send()
            to_partner(n).wait_send()
            return 0

        lax.fori_loop(0, 8, sent, 0)
        give_back(False)

    for i in range(3):
        for dx in (1, 2, 3):
            to_row(dx, i).wait_send()
        for slot in range(4):
            cross(slot, i).wait_send()
    for t in range(2):
        for e in range(2):
            pass_on(t, e, False)


W_LAG = 2


def body(queries, keys, values, frame_of_block, pair_mask, w_out):
    dma = pltpu.SemaphoreType.DMA
    wide = 3 * HD
    meta = jnp.concatenate(
        [pair_mask.reshape(-1), frame_of_block, jnp.zeros((62,), jnp.int32)]
    ).reshape(1, 128)
    return pl.pallas_call(
        kernel,
        name="frames",
        out_shape=jax.ShapeDtypeStruct((TOK, wide), jnp.bfloat16),
        in_specs=[pl.BlockSpec(memory_space=VMEM)] * 5,
        out_specs=pl.BlockSpec(memory_space=VMEM),
        scratch_shapes=[
            VMEM((4, TOK, HD), jnp.bfloat16),
            VMEM((2, 16, TOK, HD), jnp.bfloat16),
            VMEM((16, 1, 128), jnp.int32),
            pltpu.SMEM((16, 1, 128), jnp.int32),
            VMEM((2, 4, wide, wide), jnp.bfloat16),
            VMEM((4 * TOK, 2 * HD), jnp.float32),
            VMEM((4 * TOK, HD), jnp.float32),
            VMEM((4, TOK, HD), jnp.bfloat16),
            VMEM((4, 2, TOK, wide), jnp.bfloat16),
            VMEM((2, 2, TOK, wide), jnp.bfloat16),
            VMEM((4, TOK, wide), jnp.bfloat16),
            dma((3,)), dma((3, 2)), dma((3, 2, 2)), dma((16,)), dma((8,)), dma((3, 2, 4)),
            dma((4,)), dma((8,)), dma((8,)), dma((16,)), dma, dma((2, 4)), dma,
            dma((4,)), dma((4, 3)), dma((4, 3)), dma((2, 2)),
            dma((3,)), dma((4, 3)), dma((4, 3)), dma((4,)),
        ],
        compiler_params=pltpu.CompilerParams(
            collective_id=0, has_side_effects=True, vmem_limit_bytes=48 * 1024 * 1024
        ),
    )(queries, keys, values, meta, w_out)


def solution(mesh):
    return jax.shard_map(
        body,
        mesh=mesh,
        in_specs=(
            P("seq", "head"),
            P("seq", "head"),
            P("seq", "head"),
            P("seq"),
            P("seq", None),
            P("head", "seq"),
        ),
        out_specs=P("seq", "head"),
        check_vma=False,
    )
```

```python
import math

import jax
import jax.numpy as jnp
from jax import lax
from jax.experimental import pallas as pl
from jax.experimental.pallas import tpu as pltpu
from jax.sharding import PartitionSpec as P

HD = 128
BLK = 256
TOK = 512
MESH = pl.DeviceIdType.MESH
VMEM = pltpu.VMEM
FACTOR = math.log2(math.e) / math.sqrt(HD)


def remote(src, dst, send, recv, seq, head):
    return pltpu.make_async_remote_copy(
        src_ref=src, dst_ref=dst, send_sem=send, recv_sem=recv, device_id=(seq, head), device_id_type=MESH
    )


def arrived(ref, sem):
    pltpu.make_async_copy(ref, ref, sem).wait()


def chunk_owner(c, x_lo, j):
    flip = lax.rem(j, 2)
    return 2 * (2 * j + jnp.where(flip == 1, 1 - c, c)) + x_lo


def kernel(
    q, k, v, frame, pair, w, out,
    meta, mask, own, qb, kv, mt, table, wb, acc, peak, ob, a, part, got,
    s_l, s_q, s_kv, s_m, s_f, s_p, s_w, r_q, r_z, r_x, r_s, r_m, r_w, r_t,
    s_o, s_a, s_b, s_d, r_o, r_a, r_b, r_d,
):
    s, h = lax.axis_index("seq"), lax.axis_index("head")
    c = lax.rem(h, 2)
    hb = h - c
    z, x_lo = s // 2, lax.rem(s, 2)
    y, x_hi = hb // 4, lax.rem(hb, 4) // 2
    x = 2 * x_hi + x_lo
    third = lax.rem(z, 4)
    working = third < 3
    barrier = pltpu.get_barrier_semaphore()

    load_mask = pltpu.make_async_copy(pair, mask, s_l.at[0])
    load_frame = pltpu.make_async_copy(frame, own, s_l.at[1])
    load_mask.start()
    load_frame.start()

    def greet(seq, head):
        pl.semaphore_signal(barrier, inc=1, device_id=(seq, head), device_id_type=MESH)

    def greet_group(n, _):
        ps, pc = n // 2, lax.rem(n, 2)

        @pl.when(jnp.logical_not((ps == s) & (pc == c)))
        def _():
            greet(ps, hb + pc)

        return 0

    def greet_row(n, _):
        greet(2 * z + n // 2, 4 * y + 2 * (1 - x_hi) + lax.rem(n, 2))
        return 0

    def greet_line(n, _):
        py = lax.rem(y + 1 + n // 4, 4)
        greet(2 * z + lax.rem(n, 4) // 2, 4 * py + 2 * x_hi + lax.rem(n, 2))
        return 0

    lax.fori_loop(0, 32, greet_group, 0)
    lax.fori_loop(0, 4, greet_row, 0)
    lax.fori_loop(0, 12, greet_line, 0)
    load_mask.wait()
    load_frame.wait()
    lane = lax.broadcasted_iota(jnp.int32, (1, 32), 1)
    meta[0:1, 0:32] = mask[0:1, :]
    meta[0:1, 32:64] = mask[1:2, :]
    meta[0:1, 64:96] = jnp.where(lane == 0, own[0], own[1])
    pl.semaphore_wait(barrier, 47)

    def put(src, dst, send, recv, seq, head, start):
        mine = (seq == s) & (head == h)
        copy = remote(src, dst, send, recv, seq, head)
        if start:

            @pl.when(mine)
            def _():
                pltpu.make_async_copy(src, dst, recv).start()

            @pl.when(jnp.logical_not(mine))
            def _():
                copy.start()
        else:

            @pl.when(jnp.logical_not(mine))
            def _():
                copy.wait_send()

    def cols(i):
        return pl.ds(i * HD, HD)

    off = lax.rem(z - 4 * c + 8, 8)

    def order(r):
        rising = jnp.where((off == 0) | (off > 5), r, 2 - r)
        return jnp.where(off == 1, jnp.where(r == 0, 1, jnp.where(r == 1, 0, 2)), jnp.where(off == 5, jnp.where(r == 0, 0, 3 - r), rising))

    worker = lax.rem((z + 1) // 2, 2)

    def spread_meta(start):
        for r in range(3):
            pz = 4 * c + order(r)
            for px in range(2):
                for pc in range(2):
                    put(meta, mt.at[s], s_m.at[r, px, pc], r_m, 2 * pz + px, hb + pc, start)

    def spread(r, start):
        i = order(r)
        lanes = pl.ds(pl.multiple_of(i * HD, HD), HD)
        seq = 2 * (4 * c + i) + x_lo
        put(q.at[:, lanes], qb.at[z // 2], s_q.at[r], r_q.at[z // 2], seq, hb + worker, start)
        for t, src in ((0, k), (1, v)):
            put(src.at[:, lanes], kv.at[t, s], s_kv.at[r, t], r_z.at[z], seq, hb + t, start)

    def spread_w(start):
        e, r = lax.rem(z, 4) // 2, 2 * x_hi + c
        put(w, wb.at[e, r], s_w.at[4, 0, 0], r_w.at[e, r], s, 4 * y + 2 * lax.rem(z, 2) + z // 4, start)

    spread_meta(True)
    spread(0, True)
    spread_w(True)
    if not THROTTLE:
        spread(1, True)
        spread(2, True)

    def source_at(n):
        far = (n + 1) // 2
        return lax.rem(z + jnp.where(lax.rem(n, 2) == 1, far, 8 - far), 8)

    def to_sibling(piece):
        return remote(kv.at[c, piece], kv.at[c, piece], s_f.at[piece], r_s.at[piece], s, hb + 1 - c)

    def to_partner(zs):
        piece = 2 * zs + x_lo
        return remote(kv.at[c, piece], kv.at[c, piece], s_p.at[zs], r_x.at[zs], 2 * z + 1 - x_lo, h)

    def w_hop(e, r, to, slot):
        return remote(wb.at[e, r], wb.at[e, r], s_w.at[slot, e, r], r_w.at[e, r], 2 * lax.rem(z + to, 8) + x_lo, h)

    def w_each(source, relay, do):
        for e in range(2):
            far = lax.rem(z - (4 * c + 2 * e + x_hi) + 8, 8)
            for at, reach in ((0, (1, 7, 2, 6)), (2, (1, 2)), (6, (7,))):
                if source if at == 0 else relay:

                    @pl.when(far == at)
                    def _(e=e, reach=reach):
                        do(e, reach)

    def w_start(e, reach):
        for r in range(4):
            arrived(wb.at[e, r], r_w.at[e, r])
            for slot, to in enumerate(reach):
                w_hop(e, r, to, slot).start()

    def w_sent(e, reach):
        for r in range(4):
            for slot, to in enumerate(reach):
                w_hop(e, r, to, slot).wait_send()

    def w_end(e, reach):
        for r in range(4):
            arrived(wb.at[e, r], r_w.at[e, r])

    def w_rest():
        for e in range(2):
            far = lax.rem(z - (4 * c + 2 * e + x_hi) + 8, 8)

            @pl.when((far != 0) & (far != 2) & (far != 6))
            def _(e=e):
                w_end(e, ())

    def attend(piece, j, owner):
        keys = [kv[0, piece, pl.ds(u * BLK, BLK), :] for u in range(2)]
        ones = jnp.ones((BLK, HD), jnp.bfloat16)
        wide = [jnp.concatenate([kv[1, piece, pl.ds(u * BLK, BLK), :], ones], axis=1) for u in range(2)]
        for tile in range(4):
            half = tile // 2
            ok = []
            for u in range(2):
                near = (table[owner, 0, 32 * half + 2 * piece + u] == 1) & (2 * piece + u <= 2 * owner + half)
                ok.append(near | (table[piece, 0, 64 + u] == table[owner, 0, 64 + half]))
            rows = pl.ds(tile * 128, 128)
            held = pl.ds(pl.multiple_of(j * TOK + tile * 128, 128), 128)
            query = qb[j, rows, :]
            score = [
                lax.dot_general(query, keys[u], (((1,), (1,)), ((), ())), preferred_element_type=jnp.float32)
                for u in range(2)
            ]
            tops = [
                jnp.maximum(score[u][:, :HD], score[u][:, HD:]) + jnp.where(ok[u], 0.0, -1e30) for u in range(2)
            ]
            old = peak[held, :]
            new = jnp.maximum(old, jnp.max(jnp.maximum(tops[0], tops[1]), axis=1, keepdims=True))
            peak[held, :] = new
            shrink = jnp.exp2((old - new) * FACTOR)
            added = None
            for u in range(2):
                base = jnp.where(ok[u], new, 1e30)
                weight = jnp.concatenate(
                    [
                        jnp.exp2((score[u][:, cols_] - base) * FACTOR).astype(jnp.bfloat16)
                        for cols_ in (slice(0, HD), slice(HD, 2 * HD))
                    ],
                    axis=1,
                )
                dot = jnp.dot(weight, wide[u], preferred_element_type=jnp.float32)
                added = dot if added is None else added + dot
            acc[held, :HD] = acc[held, :HD] * shrink + added[:, :HD]
            acc[held, HD:] = acc[held, HD:] * shrink + added[:, HD:]

    @pl.when(working)
    def _():
        acc[...] = jnp.zeros_like(acc)
        peak[...] = jnp.full_like(peak, -1e30)

    def turn(n, _):
        for r in range(2 if THROTTLE else 0):

            @pl.when(n == THROTTLE + r)
            def _(r=r):
                spread(r, False)
                spread(r + 1, True)

        @pl.when(n == W_FROM)
        def _():
            w_each(True, False, w_start)

        @pl.when(n == W_RELAY)
        def _():
            w_each(False, True, w_start)

        @pl.when(working & (n < 8))
        def _():
            zs = source_at(n)
            piece = 2 * zs + x_lo
            arrived(kv.at[c, piece], r_z.at[zs])
            to_partner(zs).start()
            to_sibling(piece).start()

        @pl.when(working & (n > 0) & (n < 9))
        def _():
            zs = source_at(n - 1)
            piece = 2 * zs + 1 - x_lo
            arrived(kv.at[c, piece], r_x.at[zs])
            to_sibling(piece).start()

        @pl.when(working & (n == 2))
        def _():
            arrived(mt, r_m)
            local = pltpu.make_async_copy(mt, table, r_t)
            local.start()
            local.wait()

        @pl.when(working & (n > 1) & (n < 10))
        def _():
            fresh = n - 2
            zs = source_at(fresh)
            for side in range(2):
                piece = 2 * zs + side
                arrived(kv.at[1 - c, piece], r_s.at[piece])

            def chunk(j, _):
                owner = chunk_owner(c, x_lo, j)
                away = lax.rem(owner // 2 - z + 8, 8)
                since = jnp.where(away == 0, 0, jnp.where(away < 5, 2 * away - 1, 16 - 2 * away))

                @pl.when(since == fresh)
                def _():
                    arrived(qb.at[j], r_q.at[j])

                def one(m, _):
                    piece = 2 * source_at(m // 2) + lax.rem(m, 2)

                    @pl.when(piece <= owner + 2)
                    def _():
                        attend(piece, j, owner)

                    return 0

                first = jnp.where(since < fresh, fresh, jnp.where(since == fresh, 0, fresh + 1))
                lax.fori_loop(2 * first, 2 * fresh + 2, one, 0)
                return 0

            lax.fori_loop(0, 4, chunk, 0)

        return 0

    lax.fori_loop(0, 10, turn, 0)

    def give_back(j, start):
        lanes = pl.ds(pl.multiple_of(third * HD, HD), HD)
        put(ob.at[j], a.at[x, z // 4, :, lanes], s_o.at[j], r_o.at[third], chunk_owner(c, x_lo, j), hb + z // 4, start)

    @pl.when(working)
    def _():
        for j in range(4):

            def finish(n, _):
                rows = pl.ds(pl.multiple_of(j * TOK + n * 128, 128), 128)
                ob[j, pl.ds(pl.multiple_of(n * 128, 128), 128), :] = (acc[rows, :HD] / acc[rows, HD:]).astype(
                    jnp.bfloat16
                )
                return 0

            lax.fori_loop(0, 4, finish, 0)
            if j > 0:
                give_back(j - 1, True)
        give_back(3, True)

    if W_FROM > 9:
        w_each(True, False, w_start)
    if W_RELAY == 10:
        w_each(False, True, w_start)

    def cross(slot, i):
        piece = a.at[slot, c, :, cols(i)]
        return remote(piece, piece, s_b.at[slot, i], r_b.at[slot, i], s, hb + 1 - c)

    def to_row(dx, i):
        px = lax.rem(x + dx, 4)
        piece = a.at[x, c, :, cols(i)]
        return remote(piece, piece, s_a.at[dx, i], r_a.at[x, i], 2 * z + lax.rem(px, 2), 4 * y + 2 * (px // 2) + c)

    for i in range(3):
        arrived(a.at[x, c, :, cols(i)], r_o.at[i])
        for dx in (1, 3):
            to_row(dx, i).start()
        cross(x, i).start()
    for i in range(3):
        to_row(2, i).start()
    if W_RELAY > 10:
        w_each(False, True, w_start)
    w_rest()

    def gather(far):
        for i in range(3):
            for dx in far:
                slot = lax.rem(x + dx, 4)
                arrived(a.at[slot, c, :, cols(i)], r_a.at[slot, i])
                cross(slot, i).start()

    def gathered(far):
        for dx in far:
            slot = lax.rem(x + dx, 4)
            for i in range(3):
                arrived(a.at[slot, 1 - c, :, cols(i)], r_b.at[slot, i])

    def pass_on(t, e, start):
        py = 2 * c + e
        put(part.at[t, e], got.at[y], s_d.at[t, e], r_d.at[y], 2 * z + t, 4 * py + 2 * x_hi + x_lo, start)

    def multiply(t):
        for e in range(2):

            def tile(n, _):
                rows = pl.ds(pl.multiple_of(n * 128, 128), 128)
                total = None
                for r in range(4):
                    dot = jnp.dot(
                        a[2 * (r // 2) + t, r % 2, rows, :], wb[e, r], preferred_element_type=jnp.float32
                    )
                    total = dot if total is None else total + dot
                part[t, e, rows, :] = total.astype(jnp.bfloat16)
                return 0

            lax.fori_loop(0, 4, tile, 0)
            if e == 1:
                pass_on(t, 0, True)
        pass_on(t, 1, True)

    gather((3, 1))
    gathered((3, 1))
    multiply(1 - x_lo)
    gather((2,))
    gathered((2, 0))
    multiply(x_lo)
    for n in range(4):
        arrived(got.at[n], r_d.at[n])

    def add(n, _):
        rows = pl.ds(pl.multiple_of(n * 64, 64), 64)
        total = got[0, rows, :].astype(jnp.float32)
        for m in range(1, 4):
            total = total + got[m, rows, :].astype(jnp.float32)
        out[rows, :] = total.astype(jnp.bfloat16)
        return 0

    lax.fori_loop(0, 8, add, 0)

    spread_meta(False)
    spread_w(False)
    for r in range(2 if THROTTLE else 0, 3):
        spread(r, False)
    w_each(True, True, w_sent)

    @pl.when(working)
    def _():
        def sent(n, _):
            to_sibling(2 * n).wait_send()
            to_sibling(2 * n + 1).wait_send()
            to_partner(n).wait_send()
            return 0

        lax.fori_loop(0, 8, sent, 0)
        for j in range(4):
            give_back(j, False)

    for i in range(3):
        for dx in (1, 2, 3):
            to_row(dx, i).wait_send()
        for slot in range(4):
            cross(slot, i).wait_send()
    for t in range(2):
        for e in range(2):
            pass_on(t, e, False)


W_FROM = 4
W_RELAY = 10
THROTTLE = 1


def body(queries, keys, values, frame_of_block, pair_mask, w_out):
    dma = pltpu.SemaphoreType.DMA
    wide = 3 * HD
    return pl.pallas_call(
        kernel,
        name="frames",
        out_shape=jax.ShapeDtypeStruct((TOK, wide), jnp.bfloat16),
        in_specs=[pl.BlockSpec(memory_space=pl.ANY)] * 6,
        out_specs=pl.BlockSpec(memory_space=VMEM),
        scratch_shapes=[
            VMEM((1, 128), jnp.int32),
            VMEM((2, 32), jnp.int32),
            pltpu.SMEM((2,), jnp.int32),
            VMEM((4, TOK, HD), jnp.bfloat16),
            VMEM((2, 16, TOK, HD), jnp.bfloat16),
            VMEM((16, 1, 128), jnp.int32),
            pltpu.SMEM((16, 1, 128), jnp.int32),
            VMEM((2, 4, wide, wide), jnp.bfloat16),
            VMEM((4 * TOK, 2 * HD), jnp.float32),
            VMEM((4 * TOK, HD), jnp.float32),
            VMEM((4, TOK, HD), jnp.bfloat16),
            VMEM((4, 2, TOK, wide), jnp.bfloat16),
            VMEM((2, 2, TOK, wide), jnp.bfloat16),
            VMEM((4, TOK, wide), jnp.bfloat16),
            dma((2,)), dma((3,)), dma((3, 2)), dma((3, 2, 2)), dma((16,)), dma((8,)), dma((5, 2, 4)),
            dma((4,)), dma((8,)), dma((8,)), dma((16,)), dma, dma((2, 4)), dma,
            dma((4,)), dma((4, 3)), dma((4, 3)), dma((2, 2)),
            dma((3,)), dma((4, 3)), dma((4, 3)), dma((4,)),
        ],
        compiler_params=pltpu.CompilerParams(
            collective_id=0, has_side_effects=True, vmem_limit_bytes=67_000_000
        ),
    )(queries, keys, values, frame_of_block, pair_mask, w_out)


def solution(mesh):
    return jax.shard_map(
        body,
        mesh=mesh,
        in_specs=(
            P("seq", "head"),
            P("seq", "head"),
            P("seq", "head"),
            P("seq"),
            P("seq", None),
            P("head", "seq"),
        ),
        out_specs=P("seq", "head"),
        check_vma=False,
    )
```

```python
import math

import jax
import jax.numpy as jnp
from jax import lax
from jax.experimental import pallas as pl
from jax.experimental.pallas import tpu as pltpu
from jax.sharding import PartitionSpec as P

HD = 128
BLK = 256
TOK = 512
MESH = pl.DeviceIdType.MESH
VMEM = pltpu.VMEM
FACTOR = math.log2(math.e) / math.sqrt(HD)


def remote(src, dst, send, recv, seq, head):
    return pltpu.make_async_remote_copy(
        src_ref=src, dst_ref=dst, send_sem=send, recv_sem=recv, device_id=(seq, head), device_id_type=MESH
    )


def arrived(ref, sem):
    pltpu.make_async_copy(ref, ref, sem).wait()


def chunk_owner(c, x_lo, j):
    flip = lax.rem(j, 2)
    return 2 * (2 * j + jnp.where(flip == 1, 1 - c, c)) + x_lo


def kernel(
    q, k, v, frame, pair, w, out,
    meta, mask, own, qb, kv, mt, table, wb, acc, peak, ob, a, part, got,
    s_l, s_q, s_kv, s_m, s_f, s_p, s_w, r_q, r_z, r_x, r_s, r_m, r_w, r_t,
    s_o, s_a, s_b, s_d, r_o, r_a, r_b, r_d,
):
    s, h = lax.axis_index("seq"), lax.axis_index("head")
    c = lax.rem(h, 2)
    hb = h - c
    z, x_lo = s // 2, lax.rem(s, 2)
    y, x_hi = hb // 4, lax.rem(hb, 4) // 2
    x = 2 * x_hi + x_lo
    third = lax.rem(z, 4)
    working = third < 3
    barrier = pltpu.get_barrier_semaphore()

    load_mask = pltpu.make_async_copy(pair, mask, s_l.at[0])
    load_frame = pltpu.make_async_copy(frame, own, s_l.at[1])
    load_mask.start()
    load_frame.start()

    def greet(seq, head):
        pl.semaphore_signal(barrier, inc=1, device_id=(seq, head), device_id_type=MESH)

    def greet_group(n, _):
        ps, pc = n // 2, lax.rem(n, 2)

        @pl.when(jnp.logical_not((ps == s) & (pc == c)))
        def _():
            greet(ps, hb + pc)

        return 0

    def greet_row(n, _):
        greet(2 * z + n // 2, 4 * y + 2 * (1 - x_hi) + lax.rem(n, 2))
        return 0

    def greet_line(n, _):
        py = lax.rem(y + 1 + n // 4, 4)
        greet(2 * z + lax.rem(n, 4) // 2, 4 * py + 2 * x_hi + lax.rem(n, 2))
        return 0

    lax.fori_loop(0, 32, greet_group, 0)
    lax.fori_loop(0, 4, greet_row, 0)
    lax.fori_loop(0, 12, greet_line, 0)
    load_mask.wait()
    load_frame.wait()
    lane = lax.broadcasted_iota(jnp.int32, (1, 32), 1)
    meta[0:1, 0:32] = mask[0:1, :]
    meta[0:1, 32:64] = mask[1:2, :]
    meta[0:1, 64:96] = jnp.where(lane == 0, own[0], own[1])
    pl.semaphore_wait(barrier, 47)

    def put(src, dst, send, recv, seq, head, start):
        mine = (seq == s) & (head == h)
        copy = remote(src, dst, send, recv, seq, head)
        if start:

            @pl.when(mine)
            def _():
                pltpu.make_async_copy(src, dst, recv).start()

            @pl.when(jnp.logical_not(mine))
            def _():
                copy.start()
        else:

            @pl.when(jnp.logical_not(mine))
            def _():
                copy.wait_send()

    def cols(i):
        return pl.ds(i * HD, HD)

    off = lax.rem(z - 4 * c + 8, 8)

    def order(r):
        rising = jnp.where((off == 0) | (off > 5), r, 2 - r)
        return jnp.where(off == 1, jnp.where(r == 0, 1, jnp.where(r == 1, 0, 2)), jnp.where(off == 5, jnp.where(r == 0, 0, 3 - r), rising))

    worker = lax.rem((z + 1) // 2, 2)

    def spread_meta(start):
        for r in range(3):
            pz = 4 * c + order(r)
            for px in range(2):
                for pc in range(2):
                    put(meta, mt.at[s], s_m.at[r, px, pc], r_m, 2 * pz + px, hb + pc, start)

    def spread(r, start):
        i = order(2 - r if FAR_SEND else r)
        lanes = pl.ds(pl.multiple_of(i * HD, HD), HD)
        seq = 2 * (4 * c + i) + x_lo
        put(q.at[:, lanes], qb.at[z // 2], s_q.at[r], r_q.at[z // 2], seq, hb + worker, start)
        for t, src in ((0, k), (1, v)):
            put(src.at[:, lanes], kv.at[t, s], s_kv.at[r, t], r_z.at[z], seq, hb + t, start)

    def spread_w(start):
        e, r = lax.rem(z, 4) // 2, 2 * x_hi + c
        put(w, wb.at[e, r], s_w.at[4, 0, 0], r_w.at[e, r], s, 4 * y + 2 * lax.rem(z, 2) + z // 4, start)

    spread_meta(True)
    spread(0, True)
    spread_w(True)
    if not THROTTLE:
        spread(1, True)
        spread(2, True)

    def source_at(n):
        if FAR_FIRST:
            far = 4 - n // 2
            return lax.rem(z + jnp.where(n == 0, 0, jnp.where(lax.rem(n, 2) == 0, far, 8 - far)), 8)
        far = (n + 1) // 2
        return lax.rem(z + jnp.where(lax.rem(n, 2) == 1, far, 8 - far), 8)

    def to_sibling(piece):
        return remote(kv.at[c, piece], kv.at[c, piece], s_f.at[piece], r_s.at[piece], s, hb + 1 - c)

    def to_partner(zs):
        piece = 2 * zs + x_lo
        return remote(kv.at[c, piece], kv.at[c, piece], s_p.at[zs], r_x.at[zs], 2 * z + 1 - x_lo, h)

    def w_hop(e, r, to, slot):
        return remote(wb.at[e, r], wb.at[e, r], s_w.at[slot, e, r], r_w.at[e, r], 2 * lax.rem(z + to, 8) + x_lo, h)

    def w_each(source, relay, do):
        for e in range(2):
            far = lax.rem(z - (4 * c + 2 * e + x_hi) + 8, 8)
            for at, reach in ((0, (1, 7, 2, 6)), (2, (1, 2)), (6, (7,))):
                if source if at == 0 else relay:

                    @pl.when(far == at)
                    def _(e=e, reach=reach):
                        do(e, reach)

    def w_start(e, reach):
        for r in range(4):
            arrived(wb.at[e, r], r_w.at[e, r])
            for slot, to in enumerate(reach):
                w_hop(e, r, to, slot).start()

    def w_sent(e, reach):
        for r in range(4):
            for slot, to in enumerate(reach):
                w_hop(e, r, to, slot).wait_send()

    def w_end(e, reach):
        for r in range(4):
            arrived(wb.at[e, r], r_w.at[e, r])

    def w_rest():
        for e in range(2):
            far = lax.rem(z - (4 * c + 2 * e + x_hi) + 8, 8)

            @pl.when((far != 0) & (far != 2) & (far != 6))
            def _(e=e):
                w_end(e, ())

    def attend(piece, j, owner):
        keys = [kv[0, piece, pl.ds(u * BLK, BLK), :] for u in range(2)]
        ones = jnp.ones((BLK, HD), jnp.bfloat16)
        wide = [jnp.concatenate([kv[1, piece, pl.ds(u * BLK, BLK), :], ones], axis=1) for u in range(2)]
        ok = [
            [
                ((table[owner, 0, 32 * half + 2 * piece + u] == 1) & (2 * piece + u <= 2 * owner + half))
                | (table[piece, 0, 64 + u] == table[owner, 0, 64 + half])
                for u in range(2)
            ]
            for half in range(2)
        ]
        held = [pl.ds(pl.multiple_of(j * TOK + tile * 128, 128), 128) for tile in range(4)]
        scores = []
        for tile in range(4):
            query = qb[j, pl.ds(tile * 128, 128), :]
            scores.append(
                [
                    lax.dot_general(query, keys[u], (((1,), (1,)), ((), ())), preferred_element_type=jnp.float32)
                    for u in range(2)
                ]
            )
        weights = []
        for tile in range(4):
            score, seen = scores[tile], ok[tile // 2]
            tops = [
                jnp.maximum(score[u][:, :HD], score[u][:, HD:]) + jnp.where(seen[u], 0.0, -1e30) for u in range(2)
            ]
            old = peak[held[tile], :]
            new = jnp.maximum(old, jnp.max(jnp.maximum(tops[0], tops[1]), axis=1, keepdims=True))
            peak[held[tile], :] = new
            row = []
            for u in range(2):
                base = jnp.where(seen[u], new, 1e30)
                row.append(
                    jnp.concatenate(
                        [
                            jnp.exp2((score[u][:, lanes] - base) * FACTOR).astype(jnp.bfloat16)
                            for lanes in (slice(0, HD), slice(HD, 2 * HD))
                        ],
                        axis=1,
                    )
                )
            weights.append((row, jnp.exp2((old - new) * FACTOR)))
        for tile in range(4):
            row, shrink = weights[tile]
            added = jnp.dot(row[0], wide[0], preferred_element_type=jnp.float32) + jnp.dot(
                row[1], wide[1], preferred_element_type=jnp.float32
            )
            acc[held[tile], :HD] = acc[held[tile], :HD] * shrink + added[:, :HD]
            acc[held[tile], HD:] = acc[held[tile], HD:] * shrink + added[:, HD:]

    @pl.when(working)
    def _():
        acc[...] = jnp.zeros_like(acc)
        peak[...] = jnp.full_like(peak, -1e30)

    def turn(n, _):
        for r in range(2 if THROTTLE else 0):

            @pl.when(n == THROTTLE + r)
            def _(r=r):
                spread(r, False)
                spread(r + 1, True)

        @pl.when(n == W_FROM)
        def _():
            w_each(True, False, w_start)

        @pl.when(n == W_RELAY)
        def _():
            w_each(False, True, w_start)

        @pl.when(working & (n < 8))
        def _():
            zs = source_at(n)
            piece = 2 * zs + x_lo
            arrived(kv.at[c, piece], r_z.at[zs])
            to_partner(zs).start()
            to_sibling(piece).start()

        @pl.when(working & (n > 0) & (n < 9))
        def _():
            zs = source_at(n - 1)
            piece = 2 * zs + 1 - x_lo
            arrived(kv.at[c, piece], r_x.at[zs])
            to_sibling(piece).start()

        @pl.when(working & (n == 2))
        def _():
            arrived(mt, r_m)
            local = pltpu.make_async_copy(mt, table, r_t)
            local.start()
            local.wait()

        @pl.when(working & (n > 1) & (n < 10))
        def _():
            fresh = n - 2
            zs = source_at(fresh)
            for side in range(2):
                piece = 2 * zs + side
                arrived(kv.at[1 - c, piece], r_s.at[piece])

            def chunk(j, _):
                owner = chunk_owner(c, x_lo, j)
                away = lax.rem(owner // 2 - z + 8, 8)
                if FAR_FIRST:
                    since = jnp.where(away == 0, 0, jnp.where(away < 4, 8 - 2 * away, 2 * away - 7))
                else:
                    since = jnp.where(away == 0, 0, jnp.where(away < 5, 2 * away - 1, 16 - 2 * away))

                @pl.when(since == fresh)
                def _():
                    arrived(qb.at[j], r_q.at[j])

                def one(m, _):
                    piece = 2 * source_at(m // 2) + lax.rem(m, 2)

                    @pl.when(piece <= owner + 2)
                    def _():
                        attend(piece, j, owner)

                    return 0

                first = jnp.where(since < fresh, fresh, jnp.where(since == fresh, 0, fresh + 1))
                lax.fori_loop(2 * first, 2 * fresh + 2, one, 0)
                return 0

            lax.fori_loop(0, 4, chunk, 0)

        return 0

    lax.fori_loop(0, 10, turn, 0)

    def give_back(j, start):
        lanes = pl.ds(pl.multiple_of(third * HD, HD), HD)
        put(ob.at[j], a.at[x, z // 4, :, lanes], s_o.at[j], r_o.at[third], chunk_owner(c, x_lo, j), hb + z // 4, start)

    @pl.when(working)
    def _():
        for j in range(4):

            def finish(n, _):
                rows = pl.ds(pl.multiple_of(j * TOK + n * 128, 128), 128)
                ob[j, pl.ds(pl.multiple_of(n * 128, 128), 128), :] = (acc[rows, :HD] / acc[rows, HD:]).astype(
                    jnp.bfloat16
                )
                return 0

            lax.fori_loop(0, 4, finish, 0)
            if j > 0:
                give_back(j - 1, True)
        give_back(3, True)

    if W_FROM > 9:
        w_each(True, False, w_start)
    if W_RELAY == 10:
        w_each(False, True, w_start)

    def cross(slot, i):
        piece = a.at[slot, c, :, cols(i)]
        return remote(piece, piece, s_b.at[slot, i], r_b.at[slot, i], s, hb + 1 - c)

    def to_row(dx, i):
        px = lax.rem(x + dx, 4)
        piece = a.at[x, c, :, cols(i)]
        return remote(piece, piece, s_a.at[dx, i], r_a.at[x, i], 2 * z + lax.rem(px, 2), 4 * y + 2 * (px // 2) + c)

    for i in range(3):
        arrived(a.at[x, c, :, cols(i)], r_o.at[i])
        for dx in (1, 3):
            to_row(dx, i).start()
        cross(x, i).start()
    for i in range(3):
        to_row(2, i).start()
    if W_RELAY > 10:
        w_each(False, True, w_start)

    def gather(far):
        for i in range(3):
            for dx in far:
                slot = lax.rem(x + dx, 4)
                arrived(a.at[slot, c, :, cols(i)], r_a.at[slot, i])
                cross(slot, i).start()

    def gathered(far):
        for dx in far:
            slot = lax.rem(x + dx, 4)
            for i in range(3):
                arrived(a.at[slot, 1 - c, :, cols(i)], r_b.at[slot, i])

    def pass_on(t, e, start):
        py = 2 * c + e
        put(part.at[t, e], got.at[y], s_d.at[t, e], r_d.at[y], 2 * z + t, 4 * py + 2 * x_hi + x_lo, start)

    def multiply(t):
        for e in range(2):

            def tile(n, _):
                rows = pl.ds(pl.multiple_of(n * 128, 128), 128)
                total = None
                for r in range(4):
                    dot = jnp.dot(
                        a[2 * (r // 2) + t, r % 2, rows, :], wb[e, r], preferred_element_type=jnp.float32
                    )
                    total = dot if total is None else total + dot
                part[t, e, rows, :] = total.astype(jnp.bfloat16)
                return 0

            lax.fori_loop(0, 4, tile, 0)
            if e == 1:
                pass_on(t, 0, True)
        pass_on(t, 1, True)

    gather((3, 1))
    gather((2,))
    w_rest()
    gathered((3, 1))
    multiply(1 - x_lo)
    gathered((2, 0))
    multiply(x_lo)
    for n in range(4):
        arrived(got.at[n], r_d.at[n])

    def add(n, _):
        rows = pl.ds(pl.multiple_of(n * 64, 64), 64)
        total = got[0, rows, :].astype(jnp.float32)
        for m in range(1, 4):
            total = total + got[m, rows, :].astype(jnp.float32)
        out[rows, :] = total.astype(jnp.bfloat16)
        return 0

    lax.fori_loop(0, 8, add, 0)

    spread_meta(False)
    spread_w(False)
    for r in range(2 if THROTTLE else 0, 3):
        spread(r, False)
    w_each(True, True, w_sent)

    @pl.when(working)
    def _():
        def sent(n, _):
            to_sibling(2 * n).wait_send()
            to_sibling(2 * n + 1).wait_send()
            to_partner(n).wait_send()
            return 0

        lax.fori_loop(0, 8, sent, 0)
        for j in range(4):
            give_back(j, False)

    for i in range(3):
        for dx in (1, 2, 3):
            to_row(dx, i).wait_send()
        for slot in range(4):
            cross(slot, i).wait_send()
    for t in range(2):
        for e in range(2):
            pass_on(t, e, False)


W_FROM = 4
W_RELAY = 10
THROTTLE = 0
FAR_SEND = True
FAR_FIRST = True


def body(queries, keys, values, frame_of_block, pair_mask, w_out):
    dma = pltpu.SemaphoreType.DMA
    wide = 3 * HD
    return pl.pallas_call(
        kernel,
        name="frames",
        out_shape=jax.ShapeDtypeStruct((TOK, wide), jnp.bfloat16),
        in_specs=[pl.BlockSpec(memory_space=pl.ANY)] * 6,
        out_specs=pl.BlockSpec(memory_space=VMEM),
        scratch_shapes=[
            VMEM((1, 128), jnp.int32),
            VMEM((2, 32), jnp.int32),
            pltpu.SMEM((2,), jnp.int32),
            VMEM((4, TOK, HD), jnp.bfloat16),
            VMEM((2, 16, TOK, HD), jnp.bfloat16),
            VMEM((16, 1, 128), jnp.int32),
            pltpu.SMEM((16, 1, 128), jnp.int32),
            VMEM((2, 4, wide, wide), jnp.bfloat16),
            VMEM((4 * TOK, 2 * HD), jnp.float32),
            VMEM((4 * TOK, HD), jnp.float32),
            VMEM((4, TOK, HD), jnp.bfloat16),
            VMEM((4, 2, TOK, wide), jnp.bfloat16),
            VMEM((2, 2, TOK, wide), jnp.bfloat16),
            VMEM((4, TOK, wide), jnp.bfloat16),
            dma((2,)), dma((3,)), dma((3, 2)), dma((3, 2, 2)), dma((16,)), dma((8,)), dma((5, 2, 4)),
            dma((4,)), dma((8,)), dma((8,)), dma((16,)), dma, dma((2, 4)), dma,
            dma((4,)), dma((4, 3)), dma((4, 3)), dma((2, 2)),
            dma((3,)), dma((4, 3)), dma((4, 3)), dma((4,)),
        ],
        compiler_params=pltpu.CompilerParams(
            collective_id=0, has_side_effects=True, vmem_limit_bytes=67_000_000
        ),
    )(queries, keys, values, frame_of_block, pair_mask, w_out)


def solution(mesh):
    return jax.shard_map(
        body,
        mesh=mesh,
        in_specs=(
            P("seq", "head"),
            P("seq", "head"),
            P("seq", "head"),
            P("seq"),
            P("seq", None),
            P("head", "seq"),
        ),
        out_specs=P("seq", "head"),
        check_vma=False,
    )
```

```python
import math

import jax
import jax.numpy as jnp
from jax import lax
from jax.experimental import pallas as pl
from jax.experimental.pallas import tpu as pltpu
from jax.sharding import PartitionSpec as P

HD = 128
BLK = 256
TOK = 512
MESH = pl.DeviceIdType.MESH
VMEM = pltpu.VMEM
FACTOR = math.log2(math.e) / math.sqrt(HD)


def remote(src, dst, send, recv, seq, head):
    return pltpu.make_async_remote_copy(
        src_ref=src, dst_ref=dst, send_sem=send, recv_sem=recv, device_id=(seq, head), device_id_type=MESH
    )


def arrived(ref, sem):
    pltpu.make_async_copy(ref, ref, sem).wait()


def chunk_owner(c, x_lo, j):
    flip = lax.rem(j, 2)
    return 2 * (2 * j + jnp.where(flip == 1, 1 - c, c)) + x_lo


def kernel(
    q, k, v, frame, pair, w, out,
    meta, mask, own, qb, kv, mt, table, wb, acc, peak, ob, a, part, got,
    s_l, s_q, s_kv, s_m, s_f, s_p, s_w, r_q, r_z, r_x, r_s, r_m, r_w, r_t,
    s_o, s_a, s_b, s_d, r_o, r_a, r_b, r_d,
):
    s, h = lax.axis_index("seq"), lax.axis_index("head")
    c = lax.rem(h, 2)
    hb = h - c
    z, x_lo = s // 2, lax.rem(s, 2)
    y, x_hi = hb // 4, lax.rem(hb, 4) // 2
    x = 2 * x_hi + x_lo
    third = lax.rem(z, 4)
    working = third < 3
    barrier = pltpu.get_barrier_semaphore()

    load_mask = pltpu.make_async_copy(pair, mask, s_l.at[0])
    load_frame = pltpu.make_async_copy(frame, own, s_l.at[1])
    load_mask.start()
    load_frame.start()

    def greet(seq, head):
        pl.semaphore_signal(barrier, inc=1, device_id=(seq, head), device_id_type=MESH)

    def greet_group(n, _):
        ps, pc = n // 2, lax.rem(n, 2)

        @pl.when(jnp.logical_not((ps == s) & (pc == c)))
        def _():
            greet(ps, hb + pc)

        return 0

    def greet_row(n, _):
        greet(2 * z + n // 2, 4 * y + 2 * (1 - x_hi) + lax.rem(n, 2))
        return 0

    def greet_line(n, _):
        py = lax.rem(y + 1 + n // 4, 4)
        greet(2 * z + lax.rem(n, 4) // 2, 4 * py + 2 * x_hi + lax.rem(n, 2))
        return 0

    lax.fori_loop(0, 32, greet_group, 0)
    lax.fori_loop(0, 4, greet_row, 0)
    lax.fori_loop(0, 12, greet_line, 0)
    load_mask.wait()
    load_frame.wait()
    lane = lax.broadcasted_iota(jnp.int32, (1, 32), 1)
    meta[0:1, 0:32] = mask[0:1, :]
    meta[0:1, 32:64] = mask[1:2, :]
    meta[0:1, 64:96] = jnp.where(lane == 0, own[0], own[1])
    pl.semaphore_wait(barrier, 47)

    def put(src, dst, send, recv, seq, head, start):
        mine = (seq == s) & (head == h)
        copy = remote(src, dst, send, recv, seq, head)
        if start:

            @pl.when(mine)
            def _():
                pltpu.make_async_copy(src, dst, recv).start()

            @pl.when(jnp.logical_not(mine))
            def _():
                copy.start()
        else:

            @pl.when(jnp.logical_not(mine))
            def _():
                copy.wait_send()

    def cols(i):
        return pl.ds(i * HD, HD)

    off = lax.rem(z - 4 * c + 8, 8)

    def order(r):
        rising = jnp.where((off == 0) | (off > 5), r, 2 - r)
        return jnp.where(off == 1, jnp.where(r == 0, 1, jnp.where(r == 1, 0, 2)), jnp.where(off == 5, jnp.where(r == 0, 0, 3 - r), rising))

    worker = lax.rem((z + 1) // 2, 2)

    def spread_meta(start):
        for r in range(3):
            pz = 4 * c + order(r)
            for px in range(2):
                for pc in range(2):
                    put(meta, mt.at[s], s_m.at[r, px, pc], r_m, 2 * pz + px, hb + pc, start)

    def spread(r, start):
        i = order(2 - r if FAR_SEND else r)
        lanes = pl.ds(pl.multiple_of(i * HD, HD), HD)
        seq = 2 * (4 * c + i) + x_lo
        put(q.at[:, lanes], qb.at[z // 2], s_q.at[r], r_q.at[z // 2], seq, hb + worker, start)
        for t, src in ((0, k), (1, v)):
            put(src.at[:, lanes], kv.at[t, s], s_kv.at[r, t], r_z.at[z], seq, hb + t, start)

    def spread_w(start):
        e, r = lax.rem(z, 4) // 2, 2 * x_hi + c
        put(w, wb.at[e, r], s_w.at[4, 0, 0], r_w.at[e, r], s, 4 * y + 2 * lax.rem(z, 2) + z // 4, start)

    spread_meta(True)
    spread(0, True)
    spread_w(True)
    if not THROTTLE:
        spread(1, True)
        spread(2, True)

    def source_at(n):
        if FAR_FIRST:
            far = 4 - n // 2
            return lax.rem(z + jnp.where(n == 0, 0, jnp.where(lax.rem(n, 2) == 0, far, 8 - far)), 8)
        far = (n + 1) // 2
        return lax.rem(z + jnp.where(lax.rem(n, 2) == 1, far, 8 - far), 8)

    def to_sibling(piece):
        return remote(kv.at[c, piece], kv.at[c, piece], s_f.at[piece], r_s.at[piece], s, hb + 1 - c)

    def to_partner(zs):
        piece = 2 * zs + x_lo
        return remote(kv.at[c, piece], kv.at[c, piece], s_p.at[zs], r_x.at[zs], 2 * z + 1 - x_lo, h)

    def w_hop(e, r, to, slot):
        return remote(wb.at[e, r], wb.at[e, r], s_w.at[slot, e, r], r_w.at[e, r], 2 * lax.rem(z + to, 8) + x_lo, h)

    def w_each(source, relay, do):
        for e in range(2):
            far = lax.rem(z - (4 * c + 2 * e + x_hi) + 8, 8)
            for at, reach in ((0, (1, 7, 2, 6)), (2, (1, 2)), (6, (7,))):
                if source if at == 0 else relay:

                    @pl.when(far == at)
                    def _(e=e, reach=reach):
                        do(e, reach)

    def w_start(e, reach):
        for r in range(4):
            arrived(wb.at[e, r], r_w.at[e, r])
            for slot, to in enumerate(reach):
                w_hop(e, r, to, slot).start()

    def w_sent(e, reach):
        for r in range(4):
            for slot, to in enumerate(reach):
                w_hop(e, r, to, slot).wait_send()

    def w_end(e, reach):
        for r in range(4):
            arrived(wb.at[e, r], r_w.at[e, r])

    def w_rest():
        for e in range(2):
            far = lax.rem(z - (4 * c + 2 * e + x_hi) + 8, 8)

            @pl.when((far != 0) & (far != 2) & (far != 6))
            def _(e=e):
                w_end(e, ())

    def attend(piece, j, owner):
        keys = [kv[0, piece, pl.ds(u * BLK, BLK), :] for u in range(2)]
        ones = jnp.ones((BLK, HD), jnp.bfloat16)
        wide = [jnp.concatenate([kv[1, piece, pl.ds(u * BLK, BLK), :], ones], axis=1) for u in range(2)]
        ok = [
            [
                ((table[owner, 0, 32 * half + 2 * piece + u] == 1) & (2 * piece + u <= 2 * owner + half))
                | (table[piece, 0, 64 + u] == table[owner, 0, 64 + half])
                for u in range(2)
            ]
            for half in range(2)
        ]
        held = [pl.ds(pl.multiple_of(j * TOK + tile * 128, 128), 128) for tile in range(4)]
        scores = []
        for tile in range(4):
            query = qb[j, pl.ds(tile * 128, 128), :]
            scores.append(
                [
                    lax.dot_general(query, keys[u], (((1,), (1,)), ((), ())), preferred_element_type=jnp.float32)
                    for u in range(2)
                ]
            )
        weights = []
        for tile in range(4):
            score, seen = scores[tile], ok[tile // 2]
            tops = [
                jnp.maximum(score[u][:, :HD], score[u][:, HD:]) + jnp.where(seen[u], 0.0, -1e30) for u in range(2)
            ]
            old = peak[held[tile], :]
            new = jnp.maximum(old, jnp.max(jnp.maximum(tops[0], tops[1]), axis=1, keepdims=True))
            peak[held[tile], :] = new
            row = []
            for u in range(2):
                base = jnp.where(seen[u], new, 1e30)
                row.append(
                    jnp.concatenate(
                        [
                            jnp.exp2((score[u][:, lanes] - base) * FACTOR).astype(jnp.bfloat16)
                            for lanes in (slice(0, HD), slice(HD, 2 * HD))
                        ],
                        axis=1,
                    )
                )
            weights.append((row, jnp.exp2((old - new) * FACTOR)))
        for tile in range(4):
            row, shrink = weights[tile]
            added = jnp.dot(row[0], wide[0], preferred_element_type=jnp.float32) + jnp.dot(
                row[1], wide[1], preferred_element_type=jnp.float32
            )
            acc[held[tile], :HD] = acc[held[tile], :HD] * shrink + added[:, :HD]
            acc[held[tile], HD:] = acc[held[tile], HD:] * shrink + added[:, HD:]

    @pl.when(working)
    def _():
        acc[...] = jnp.zeros_like(acc)
        peak[...] = jnp.full_like(peak, -1e30)

    def turn(n, _):
        for r in range(2 if THROTTLE else 0):

            @pl.when(n == THROTTLE + r)
            def _(r=r):
                spread(r, False)
                spread(r + 1, True)

        @pl.when((n == W_FROM) & jnp.logical_not(working))
        def _():
            for r in range(2 if THROTTLE else 0, 3):
                spread(r, False)

        @pl.when(n == W_FROM)
        def _():
            w_each(True, False, w_start)

        @pl.when(n == W_RELAY)
        def _():
            w_each(False, True, w_start)

        @pl.when(working & (n < 8))
        def _():
            zs = source_at(n)
            piece = 2 * zs + x_lo
            arrived(kv.at[c, piece], r_z.at[zs])
            to_partner(zs).start()
            to_sibling(piece).start()

        @pl.when(working & (n > 0) & (n < 9))
        def _():
            zs = source_at(n - 1)
            piece = 2 * zs + 1 - x_lo
            arrived(kv.at[c, piece], r_x.at[zs])
            to_sibling(piece).start()

        @pl.when(working & (n == 2))
        def _():
            arrived(mt, r_m)
            local = pltpu.make_async_copy(mt, table, r_t)
            local.start()
            local.wait()

        @pl.when(working & (n > 1) & (n < 10))
        def _():
            fresh = n - 2
            zs = source_at(fresh)
            for side in range(2):
                piece = 2 * zs + side
                arrived(kv.at[1 - c, piece], r_s.at[piece])

            def chunk(j, _):
                owner = chunk_owner(c, x_lo, j)
                away = lax.rem(owner // 2 - z + 8, 8)
                if FAR_FIRST:
                    since = jnp.where(away == 0, 0, jnp.where(away < 4, 8 - 2 * away, 2 * away - 7))
                else:
                    since = jnp.where(away == 0, 0, jnp.where(away < 5, 2 * away - 1, 16 - 2 * away))

                @pl.when(since == fresh)
                def _():
                    arrived(qb.at[j], r_q.at[j])

                def one(m, _):
                    piece = 2 * source_at(m // 2) + lax.rem(m, 2)

                    @pl.when(piece <= owner + 2)
                    def _():
                        attend(piece, j, owner)

                    return 0

                first = jnp.where(since < fresh, fresh, jnp.where(since == fresh, 0, fresh + 1))
                lax.fori_loop(2 * first, 2 * fresh + 2, one, 0)
                return 0

            lax.fori_loop(0, 4, chunk, 0)

        return 0

    lax.fori_loop(0, 10, turn, 0)

    def give_back(j, start):
        lanes = pl.ds(pl.multiple_of(third * HD, HD), HD)
        put(ob.at[j], a.at[x, z // 4, :, lanes], s_o.at[j], r_o.at[third], chunk_owner(c, x_lo, j), hb + z // 4, start)

    @pl.when(working)
    def _():
        for j in range(4):

            def finish(n, _):
                rows = pl.ds(pl.multiple_of(j * TOK + n * 128, 128), 128)
                ob[j, pl.ds(pl.multiple_of(n * 128, 128), 128), :] = (acc[rows, :HD] / acc[rows, HD:]).astype(
                    jnp.bfloat16
                )
                return 0

            lax.fori_loop(0, 4, finish, 0)
            if j > 0:
                give_back(j - 1, True)
        give_back(3, True)

    if W_FROM > 9:
        w_each(True, False, w_start)
    if W_RELAY == 10:
        w_each(False, True, w_start)

    def cross(slot, i):
        piece = a.at[slot, c, :, cols(i)]
        return remote(piece, piece, s_b.at[slot, i], r_b.at[slot, i], s, hb + 1 - c)

    def to_row(dx, i):
        px = lax.rem(x + dx, 4)
        piece = a.at[x, c, :, cols(i)]
        return remote(piece, piece, s_a.at[dx, i], r_a.at[x, i], 2 * z + lax.rem(px, 2), 4 * y + 2 * (px // 2) + c)

    def relay(i):
        right = i + c < 2
        slot = lax.rem(jnp.where(right, x + 3, x + 1), 4)
        px = lax.rem(jnp.where(right, x + 1, x + 3), 4)
        piece = a.at[slot, c, :, cols(i)]
        return remote(
            piece, piece, s_a.at[2, i], r_a.at[slot, i], 2 * z + lax.rem(px, 2), 4 * y + 2 * (px // 2) + c
        )

    for i in range(3):
        arrived(a.at[x, c, :, cols(i)], r_o.at[i])
        for dx in (1, 3):
            to_row(dx, i).start()
        cross(x, i).start()
    if W_RELAY > 10:
        w_each(False, True, w_start)

    def gather(far):
        for i in range(3):
            for dx in far:
                slot = lax.rem(x + dx, 4)
                arrived(a.at[slot, c, :, cols(i)], r_a.at[slot, i])
                if dx != 2:

                    @pl.when((i + c < 2) if dx == 3 else (i + c > 1))
                    def _():
                        relay(i).start()

                cross(slot, i).start()

    def gathered(far):
        for dx in far:
            slot = lax.rem(x + dx, 4)
            for i in range(3):
                arrived(a.at[slot, 1 - c, :, cols(i)], r_b.at[slot, i])

    def pass_on(t, e, start):
        py = 2 * c + e
        put(part.at[t, e], got.at[y], s_d.at[t, e], r_d.at[y], 2 * z + t, 4 * py + 2 * x_hi + x_lo, start)

    def multiply(t):
        for e in range(2):

            def tile(n, _):
                rows = pl.ds(pl.multiple_of(n * M_TILE, M_TILE), M_TILE)
                total = None
                for r in range(4):
                    dot = jnp.dot(
                        a[2 * (r // 2) + t, r % 2, rows, :], wb[e, r], preferred_element_type=jnp.float32
                    )
                    total = dot if total is None else total + dot
                part[t, e, rows, :] = total.astype(jnp.bfloat16)
                return 0

            lax.fori_loop(0, TOK // M_TILE, tile, 0)
            if e == 1:
                pass_on(t, 0, True)
        pass_on(t, 1, True)

    gather((3, 1))
    gather((2,))
    w_rest()
    gathered((3, 1))
    multiply(1 - x_lo)
    gathered((2, 0))
    multiply(x_lo)
    for n in range(4):
        arrived(got.at[n], r_d.at[n])

    def add(n, _):
        rows = pl.ds(pl.multiple_of(n * 64, 64), 64)
        total = got[0, rows, :].astype(jnp.float32)
        for m in range(1, 4):
            total = total + got[m, rows, :].astype(jnp.float32)
        out[rows, :] = total.astype(jnp.bfloat16)
        return 0

    lax.fori_loop(0, 8, add, 0)

    spread_meta(False)
    spread_w(False)

    @pl.when(working)
    def _():
        for r in range(2 if THROTTLE else 0, 3):
            spread(r, False)

    w_each(True, True, w_sent)

    @pl.when(working)
    def _():
        def sent(n, _):
            to_sibling(2 * n).wait_send()
            to_sibling(2 * n + 1).wait_send()
            to_partner(n).wait_send()
            return 0

        lax.fori_loop(0, 8, sent, 0)
        for j in range(4):
            give_back(j, False)

    for i in range(3):
        for dx in (1, 3):
            to_row(dx, i).wait_send()
        relay(i).wait_send()
        for slot in range(4):
            cross(slot, i).wait_send()
    for t in range(2):
        for e in range(2):
            pass_on(t, e, False)


W_FROM = 4
M_TILE = 512
W_RELAY = 10
THROTTLE = 0
FAR_SEND = True
FAR_FIRST = True


def body(queries, keys, values, frame_of_block, pair_mask, w_out):
    dma = pltpu.SemaphoreType.DMA
    wide = 3 * HD
    return pl.pallas_call(
        kernel,
        name="frames",
        out_shape=jax.ShapeDtypeStruct((TOK, wide), jnp.bfloat16),
        in_specs=[pl.BlockSpec(memory_space=pl.ANY)] * 6,
        out_specs=pl.BlockSpec(memory_space=VMEM),
        scratch_shapes=[
            VMEM((1, 128), jnp.int32),
            VMEM((2, 32), jnp.int32),
            pltpu.SMEM((2,), jnp.int32),
            VMEM((4, TOK, HD), jnp.bfloat16),
            VMEM((2, 16, TOK, HD), jnp.bfloat16),
            VMEM((16, 1, 128), jnp.int32),
            pltpu.SMEM((16, 1, 128), jnp.int32),
            VMEM((2, 4, wide, wide), jnp.bfloat16),
            VMEM((4 * TOK, 2 * HD), jnp.float32),
            VMEM((4 * TOK, HD), jnp.float32),
            VMEM((4, TOK, HD), jnp.bfloat16),
            VMEM((4, 2, TOK, wide), jnp.bfloat16),
            VMEM((2, 2, TOK, wide), jnp.bfloat16),
            VMEM((4, TOK, wide), jnp.bfloat16),
            dma((2,)), dma((3,)), dma((3, 2)), dma((3, 2, 2)), dma((16,)), dma((8,)), dma((5, 2, 4)),
            dma((4,)), dma((8,)), dma((8,)), dma((16,)), dma, dma((2, 4)), dma,
            dma((4,)), dma((4, 3)), dma((4, 3)), dma((2, 2)),
            dma((3,)), dma((4, 3)), dma((4, 3)), dma((4,)),
        ],
        compiler_params=pltpu.CompilerParams(
            collective_id=0, has_side_effects=True, vmem_limit_bytes=67_000_000
        ),
    )(queries, keys, values, frame_of_block, pair_mask, w_out)


def solution(mesh):
    return jax.shard_map(
        body,
        mesh=mesh,
        in_specs=(
            P("seq", "head"),
            P("seq", "head"),
            P("seq", "head"),
            P("seq"),
            P("seq", None),
            P("head", "seq"),
        ),
        out_specs=P("seq", "head"),
        check_vma=False,
    )
```

```python
import math

import jax
import jax.numpy as jnp
from jax import lax
from jax.experimental import pallas as pl
from jax.experimental.pallas import tpu as pltpu
from jax.sharding import PartitionSpec as P

HD = 128
BLK = 256
TOK = 512
MESH = pl.DeviceIdType.MESH
VMEM = pltpu.VMEM
FACTOR = math.log2(math.e) / math.sqrt(HD)


def remote(src, dst, send, recv, seq, head):
    return pltpu.make_async_remote_copy(
        src_ref=src, dst_ref=dst, send_sem=send, recv_sem=recv, device_id=(seq, head), device_id_type=MESH
    )


def arrived(ref, sem):
    pltpu.make_async_copy(ref, ref, sem).wait()


def chunk_owner(c, x_lo, j):
    flip = lax.rem(j, 2)
    return 2 * (2 * j + jnp.where(flip == 1, 1 - c, c)) + x_lo


def kernel(
    q, k, v, frame, pair, w, out,
    meta, mask, own, qb, kv, mt, table, wb, acc, peak, ob, a, part, got,
    s_l, s_q, s_kv, s_m, s_f, s_p, s_w, r_q, r_z, r_x, r_s, r_m, r_w, r_t,
    s_o, s_a, s_b, s_d, r_o, r_a, r_b, r_d,
):
    s, h = lax.axis_index("seq"), lax.axis_index("head")
    c = lax.rem(h, 2)
    hb = h - c
    z, x_lo = s // 2, lax.rem(s, 2)
    y, x_hi = hb // 4, lax.rem(hb, 4) // 2
    x = 2 * x_hi + x_lo
    third = lax.rem(z, 4)
    working = third < 3
    barrier = pltpu.get_barrier_semaphore()

    load_mask = pltpu.make_async_copy(pair, mask, s_l.at[0])
    load_frame = pltpu.make_async_copy(frame, own, s_l.at[1])
    load_mask.start()
    load_frame.start()

    def greet(seq, head):
        pl.semaphore_signal(barrier, inc=1, device_id=(seq, head), device_id_type=MESH)

    def greet_group(n, _):
        ps, pc = n // 2, lax.rem(n, 2)

        @pl.when(jnp.logical_not((ps == s) & (pc == c)))
        def _():
            greet(ps, hb + pc)

        return 0

    def greet_row(n, _):
        greet(2 * z + n // 2, 4 * y + 2 * (1 - x_hi) + lax.rem(n, 2))
        return 0

    def greet_line(n, _):
        py = lax.rem(y + 1 + n // 4, 4)
        greet(2 * z + lax.rem(n, 4) // 2, 4 * py + 2 * x_hi + lax.rem(n, 2))
        return 0

    lax.fori_loop(0, 32, greet_group, 0)
    lax.fori_loop(0, 4, greet_row, 0)
    lax.fori_loop(0, 12, greet_line, 0)
    load_mask.wait()
    load_frame.wait()
    lane = lax.broadcasted_iota(jnp.int32, (1, 32), 1)
    meta[0:1, 0:32] = mask[0:1, :]
    meta[0:1, 32:64] = mask[1:2, :]
    meta[0:1, 64:96] = jnp.where(lane == 0, own[0], own[1])
    pl.semaphore_wait(barrier, 47)

    def put(src, dst, send, recv, seq, head, start):
        mine = (seq == s) & (head == h)
        copy = remote(src, dst, send, recv, seq, head)
        if start:

            @pl.when(mine)
            def _():
                pltpu.make_async_copy(src, dst, recv).start()

            @pl.when(jnp.logical_not(mine))
            def _():
                copy.start()
        else:

            @pl.when(jnp.logical_not(mine))
            def _():
                copy.wait_send()

    def cols(i):
        return pl.ds(i * HD, HD)

    off = lax.rem(z - 4 * c + 8, 8)

    def order(r):
        rising = jnp.where((off == 0) | (off > 5), r, 2 - r)
        return jnp.where(off == 1, jnp.where(r == 0, 1, jnp.where(r == 1, 0, 2)), jnp.where(off == 5, jnp.where(r == 0, 0, 3 - r), rising))

    worker = lax.rem((z + 1) // 2, 2)

    def spread_meta(start):
        for r in range(3):
            pz = 4 * c + order(r)
            for px in range(2):
                for pc in range(2):
                    put(meta, mt.at[s], s_m.at[r, px, pc], r_m, 2 * pz + px, hb + pc, start)

    def spread(r, start):
        i = order(2 - r if FAR_SEND else r)
        lanes = pl.ds(pl.multiple_of(i * HD, HD), HD)
        seq = 2 * (4 * c + i) + x_lo
        put(q.at[:, lanes], qb.at[z // 2], s_q.at[r], r_q.at[z // 2], seq, hb + worker, start)
        for t, src in ((0, k), (1, v)):
            put(src.at[:, lanes], kv.at[t, s], s_kv.at[r, t], r_z.at[z], seq, hb + t, start)

    def spread_w(start):
        e, r = lax.rem(z, 4) // 2, 2 * x_hi + c
        put(w, wb.at[e, r], s_w.at[4, 0, 0], r_w.at[e, r], s, 4 * y + 2 * lax.rem(z, 2) + z // 4, start)

    spread_meta(True)
    spread(0, True)
    spread_w(True)
    if not THROTTLE:
        spread(1, True)
        spread(2, True)

    def source_at(n):
        if FAR_FIRST:
            far = 4 - n // 2
            return lax.rem(z + jnp.where(n == 0, 0, jnp.where(lax.rem(n, 2) == 0, far, 8 - far)), 8)
        far = (n + 1) // 2
        return lax.rem(z + jnp.where(lax.rem(n, 2) == 1, far, 8 - far), 8)

    def to_sibling(piece):
        return remote(kv.at[c, piece], kv.at[c, piece], s_f.at[piece], r_s.at[piece], s, hb + 1 - c)

    def to_partner(zs):
        piece = 2 * zs + x_lo
        return remote(kv.at[c, piece], kv.at[c, piece], s_p.at[zs], r_x.at[zs], 2 * z + 1 - x_lo, h)

    def w_hop(e, r, to, slot):
        return remote(wb.at[e, r], wb.at[e, r], s_w.at[slot, e, r], r_w.at[e, r], 2 * lax.rem(z + to, 8) + x_lo, h)

    def w_each(source, relay, do):
        for e in range(2):
            far = lax.rem(z - (4 * c + 2 * e + x_hi) + 8, 8)
            for at, reach in ((0, (1, 7, 2, 6)), (2, (1, 2)), (6, (7,))):
                if source if at == 0 else relay:

                    @pl.when(far == at)
                    def _(e=e, reach=reach):
                        do(e, reach)

    def w_start(e, reach):
        for r in range(4):
            arrived(wb.at[e, r], r_w.at[e, r])
            for slot, to in enumerate(reach):
                w_hop(e, r, to, slot).start()

    def w_sent(e, reach):
        for r in range(4):
            for slot, to in enumerate(reach):
                w_hop(e, r, to, slot).wait_send()

    def w_end(e, reach):
        for r in range(4):
            arrived(wb.at[e, r], r_w.at[e, r])

    def w_rest(e):
        far = lax.rem(z - (4 * c + 2 * e + x_hi) + 8, 8)

        @pl.when((far != 0) & (far != 2) & (far != 6))
        def _():
            w_end(e, ())

    def attend(piece, j, owner):
        keys = [kv[0, piece, pl.ds(u * BLK, BLK), :] for u in range(2)]
        ones = jnp.ones((BLK, HD), jnp.bfloat16)
        wide = [jnp.concatenate([kv[1, piece, pl.ds(u * BLK, BLK), :], ones], axis=1) for u in range(2)]
        ok = [
            [
                ((table[owner, 0, 32 * half + 2 * piece + u] == 1) & (2 * piece + u <= 2 * owner + half))
                | (table[piece, 0, 64 + u] == table[owner, 0, 64 + half])
                for u in range(2)
            ]
            for half in range(2)
        ]
        held = [pl.ds(pl.multiple_of(j * TOK + tile * 128, 128), 128) for tile in range(4)]
        scores = []
        for tile in range(4):
            query = qb[j, pl.ds(tile * 128, 128), :]
            scores.append(
                [
                    lax.dot_general(query, keys[u], (((1,), (1,)), ((), ())), preferred_element_type=jnp.float32)
                    for u in range(2)
                ]
            )
        weights = []
        for tile in range(4):
            score, seen = scores[tile], ok[tile // 2]
            tops = [
                jnp.maximum(score[u][:, :HD], score[u][:, HD:]) + jnp.where(seen[u], 0.0, -1e30) for u in range(2)
            ]
            old = peak[held[tile], :]
            new = jnp.maximum(old, jnp.max(jnp.maximum(tops[0], tops[1]), axis=1, keepdims=True))
            peak[held[tile], :] = new
            row = []
            for u in range(2):
                base = jnp.where(seen[u], new, 1e30)
                row.append(
                    jnp.concatenate(
                        [
                            jnp.exp2((score[u][:, lanes] - base) * FACTOR).astype(jnp.bfloat16)
                            for lanes in (slice(0, HD), slice(HD, 2 * HD))
                        ],
                        axis=1,
                    )
                )
            weights.append((row, jnp.exp2((old - new) * FACTOR)))
        for tile in range(4):
            row, shrink = weights[tile]
            added = jnp.dot(row[0], wide[0], preferred_element_type=jnp.float32) + jnp.dot(
                row[1], wide[1], preferred_element_type=jnp.float32
            )
            acc[held[tile], :HD] = acc[held[tile], :HD] * shrink + added[:, :HD]
            acc[held[tile], HD:] = acc[held[tile], HD:] * shrink + added[:, HD:]

    @pl.when(working)
    def _():
        acc[...] = jnp.zeros_like(acc)
        peak[...] = jnp.full_like(peak, -1e30)

    def turn(n, _):
        for r in range(2 if THROTTLE else 0):

            @pl.when(n == THROTTLE + r)
            def _(r=r):
                spread(r, False)
                spread(r + 1, True)

        @pl.when((n == W_FROM) & jnp.logical_not(working))
        def _():
            for r in range(2 if THROTTLE else 0, 3):
                spread(r, False)

        @pl.when(n == W_FROM)
        def _():
            w_each(True, False, w_start)

        @pl.when(n == W_RELAY)
        def _():
            w_each(False, True, w_start)

        @pl.when(working & (n < 8))
        def _():
            zs = source_at(n)
            piece = 2 * zs + x_lo
            arrived(kv.at[c, piece], r_z.at[zs])
            to_partner(zs).start()
            to_sibling(piece).start()

        @pl.when(working & (n > 0) & (n < 9))
        def _():
            zs = source_at(n - 1)
            piece = 2 * zs + 1 - x_lo
            arrived(kv.at[c, piece], r_x.at[zs])
            to_sibling(piece).start()

        @pl.when(working & (n == 2))
        def _():
            arrived(mt, r_m)
            local = pltpu.make_async_copy(mt, table, r_t)
            local.start()
            local.wait()

        @pl.when(working & (n > 1) & (n < 10))
        def _():
            fresh = n - 2
            zs = source_at(fresh)
            for side in range(2):
                piece = 2 * zs + side
                arrived(kv.at[1 - c, piece], r_s.at[piece])

            def chunk(j, _):
                owner = chunk_owner(c, x_lo, j)
                away = lax.rem(owner // 2 - z + 8, 8)
                if FAR_FIRST:
                    since = jnp.where(away == 0, 0, jnp.where(away < 4, 8 - 2 * away, 2 * away - 7))
                else:
                    since = jnp.where(away == 0, 0, jnp.where(away < 5, 2 * away - 1, 16 - 2 * away))

                @pl.when(since == fresh)
                def _():
                    arrived(qb.at[j], r_q.at[j])

                def one(m, _):
                    piece = 2 * source_at(m // 2) + lax.rem(m, 2)

                    @pl.when(piece <= owner + 2)
                    def _():
                        attend(piece, j, owner)

                    return 0

                first = jnp.where(since < fresh, fresh, jnp.where(since == fresh, 0, fresh + 1))
                lax.fori_loop(2 * first, 2 * fresh + 2, one, 0)
                return 0

            lax.fori_loop(0, 4, chunk, 0)

        return 0

    lax.fori_loop(0, 10, turn, 0)

    def give_back(j, start):
        lanes = pl.ds(pl.multiple_of(third * HD, HD), HD)
        put(ob.at[j], a.at[x, z // 4, :, lanes], s_o.at[j], r_o.at[third], chunk_owner(c, x_lo, j), hb + z // 4, start)

    @pl.when(working)
    def _():
        for j in range(4):

            def finish(n, _):
                rows = pl.ds(pl.multiple_of(j * TOK + n * 128, 128), 128)
                ob[j, pl.ds(pl.multiple_of(n * 128, 128), 128), :] = (acc[rows, :HD] / acc[rows, HD:]).astype(
                    jnp.bfloat16
                )
                return 0

            lax.fori_loop(0, 4, finish, 0)
            if j > 0:
                give_back(j - 1, True)
        give_back(3, True)

    if W_FROM > 9:
        w_each(True, False, w_start)
    if W_RELAY == 10:
        w_each(False, True, w_start)

    def cross(slot, i):
        piece = a.at[slot, c, :, cols(i)]
        return remote(piece, piece, s_b.at[slot, i], r_b.at[slot, i], s, hb + 1 - c)

    def to_row(dx, i):
        px = lax.rem(x + dx, 4)
        piece = a.at[x, c, :, cols(i)]
        return remote(piece, piece, s_a.at[dx, i], r_a.at[x, i], 2 * z + lax.rem(px, 2), 4 * y + 2 * (px // 2) + c)

    def relay(i):
        right = i + c < 2
        slot = lax.rem(jnp.where(right, x + 3, x + 1), 4)
        px = lax.rem(jnp.where(right, x + 1, x + 3), 4)
        piece = a.at[slot, c, :, cols(i)]
        return remote(
            piece, piece, s_a.at[2, i], r_a.at[slot, i], 2 * z + lax.rem(px, 2), 4 * y + 2 * (px // 2) + c
        )

    for i in range(3):
        arrived(a.at[x, c, :, cols(i)], r_o.at[i])
        for dx in (1, 3):
            to_row(dx, i).start()
        cross(x, i).start()
    if W_RELAY > 10:
        w_each(False, True, w_start)

    def gather(far):
        for i in range(3):
            for dx in far:
                slot = lax.rem(x + dx, 4)
                arrived(a.at[slot, c, :, cols(i)], r_a.at[slot, i])
                if dx != 2:

                    @pl.when((i + c < 2) if dx == 3 else (i + c > 1))
                    def _():
                        relay(i).start()

                cross(slot, i).start()

    def gathered(far):
        for dx in far:
            slot = lax.rem(x + dx, 4)
            for i in range(3):
                arrived(a.at[slot, 1 - c, :, cols(i)], r_b.at[slot, i])

    def pass_on(t, e, start):
        py = 2 * c + e
        put(part.at[t, e], got.at[y], s_d.at[t, e], r_d.at[y], 2 * z + t, 4 * py + 2 * x_hi + x_lo, start)

    def multiply(t, e):
        def tile(n, _):
            rows = pl.ds(pl.multiple_of(n * M_TILE, M_TILE), M_TILE)
            total = None
            for r in range(4):
                dot = jnp.dot(
                    a[2 * (r // 2) + t, r % 2, rows, :], wb[e, r], preferred_element_type=jnp.float32
                )
                total = dot if total is None else total + dot
            part[t, e, rows, :] = total.astype(jnp.bfloat16)
            return 0

        lax.fori_loop(0, TOK // M_TILE, tile, 0)

    gather((3, 1))
    gather((2,))
    w_rest(0)
    gathered((3, 1))
    multiply(1 - x_lo, 0)
    gathered((2, 0))
    multiply(x_lo, 0)
    pass_on(1 - x_lo, 0, True)
    w_rest(1)
    pass_on(x_lo, 0, True)
    multiply(1 - x_lo, 1)
    multiply(x_lo, 1)
    pass_on(1 - x_lo, 1, True)
    pass_on(x_lo, 1, True)
    for n in range(4):
        arrived(got.at[n], r_d.at[n])

    def add(n, _):
        rows = pl.ds(pl.multiple_of(n * 64, 64), 64)
        total = got[0, rows, :].astype(jnp.float32)
        for m in range(1, 4):
            total = total + got[m, rows, :].astype(jnp.float32)
        out[rows, :] = total.astype(jnp.bfloat16)
        return 0

    lax.fori_loop(0, 8, add, 0)

    spread_meta(False)
    spread_w(False)

    @pl.when(working)
    def _():
        for r in range(2 if THROTTLE else 0, 3):
            spread(r, False)

    w_each(True, True, w_sent)

    @pl.when(working)
    def _():
        def sent(n, _):
            to_sibling(2 * n).wait_send()
            to_sibling(2 * n + 1).wait_send()
            to_partner(n).wait_send()
            return 0

        lax.fori_loop(0, 8, sent, 0)
        for j in range(4):
            give_back(j, False)

    for i in range(3):
        for dx in (1, 3):
            to_row(dx, i).wait_send()
        relay(i).wait_send()
        for slot in range(4):
            cross(slot, i).wait_send()
    for t in range(2):
        for e in range(2):
            pass_on(t, e, False)


W_FROM = 4
M_TILE = 512
W_RELAY = 10
THROTTLE = 0
FAR_SEND = True
FAR_FIRST = True


def body(queries, keys, values, frame_of_block, pair_mask, w_out):
    dma = pltpu.SemaphoreType.DMA
    wide = 3 * HD
    return pl.pallas_call(
        kernel,
        name="frames",
        out_shape=jax.ShapeDtypeStruct((TOK, wide), jnp.bfloat16),
        in_specs=[pl.BlockSpec(memory_space=pl.ANY)] * 6,
        out_specs=pl.BlockSpec(memory_space=VMEM),
        scratch_shapes=[
            VMEM((1, 128), jnp.int32),
            VMEM((2, 32), jnp.int32),
            pltpu.SMEM((2,), jnp.int32),
            VMEM((4, TOK, HD), jnp.bfloat16),
            VMEM((2, 16, TOK, HD), jnp.bfloat16),
            VMEM((16, 1, 128), jnp.int32),
            pltpu.SMEM((16, 1, 128), jnp.int32),
            VMEM((2, 4, wide, wide), jnp.bfloat16),
            VMEM((4 * TOK, 2 * HD), jnp.float32),
            VMEM((4 * TOK, HD), jnp.float32),
            VMEM((4, TOK, HD), jnp.bfloat16),
            VMEM((4, 2, TOK, wide), jnp.bfloat16),
            VMEM((2, 2, TOK, wide), jnp.bfloat16),
            VMEM((4, TOK, wide), jnp.bfloat16),
            dma((2,)), dma((3,)), dma((3, 2)), dma((3, 2, 2)), dma((16,)), dma((8,)), dma((5, 2, 4)),
            dma((4,)), dma((8,)), dma((8,)), dma((16,)), dma, dma((2, 4)), dma,
            dma((4,)), dma((4, 3)), dma((4, 3)), dma((2, 2)),
            dma((3,)), dma((4, 3)), dma((4, 3)), dma((4,)),
        ],
        compiler_params=pltpu.CompilerParams(
            collective_id=0, has_side_effects=True, vmem_limit_bytes=67_000_000
        ),
    )(queries, keys, values, frame_of_block, pair_mask, w_out)


def solution(mesh):
    return jax.shard_map(
        body,
        mesh=mesh,
        in_specs=(
            P("seq", "head"),
            P("seq", "head"),
            P("seq", "head"),
            P("seq"),
            P("seq", None),
            P("head", "seq"),
        ),
        out_specs=P("seq", "head"),
        check_vma=False,
    )
```
